256 devices in a mesh: seq: 64 (over x, z, core), head: 4 (over y).
Axes of the slice: x: 4, y: 4, z: 8, core: 2. Of those that a mesh axis runs over, the one named last changes fastest.
Arguments:
- inputs: float32 [32768, 5120], P('seq', 'head'), may hold values from -3 to 3
- log_decay: float32 [80, 32768], P('head', 'seq'), may hold values from -1 to 0, as said below
- b_proj: float32 [32768, 128], P('seq'), may hold values from -0.5 to 0.5
- c_proj: float32 [32768, 128], P('seq'), may hold values from -0.5 to 0.5
- entry_states: float32 [64, 80, 64, 128], P('seq', 'head'), may hold values from -12 to 12
- out_grad: float32 [32768, 5120], P('seq', 'head'), may hold values from -3 to 3
Outputs:
- d_inputs: float32 [32768, 5120], P('seq', 'head')
- d_log_decay: float32 [80, 32768], P('head', 'seq')
- d_b_proj: float32 [32768, 128], P('seq')
- d_c_proj: float32 [32768, 128], P('seq')
- entry_grad: float32 [64, 80, 64, 128], P('seq', 'head')
The draws below stay inside these ranges and needn't reach their ends.
Inputs may be any that keep to these rules, and one draw needn't show every extreme that they name: `log_decay`: negative everywhere.
All inputs are finite; a program needn't handle non-finite values.
Results may differ from the reference program's by a relative error of at most 0.0003.
Values sent between devices are 32-bit elements; how exact they have to be, the bound alone decides.
A program may use at most 192 MiB of HBM per device.

```python
import jax
import jax.numpy as jnp
from jax import lax

HEAD_TOTAL = 80
HEAD_DIM = 64
D_STATE = 128
BLOCK = 256
TOK_DEV = 512
SHARDS = 64
TOKEN_TOTAL = 32768


def draw_log_decay(key, part):
    random_key_list = jax.random.split(key, 11)
    shard_count = TOKEN_TOTAL // TOK_DEV
    fast_count = max(1, HEAD_TOTAL // 5)
    medium_count = max(1, 3 * HEAD_TOTAL // 10)
    head_rank = jax.random.permutation(random_key_list[0], HEAD_TOTAL)
    fast_flag = head_rank < fast_count
    medium_flag = (head_rank >= fast_count) & (head_rank < fast_count + medium_count)
    slow_flag = head_rank >= fast_count + medium_count
    fast_rate = jax.random.uniform(random_key_list[1], (HEAD_TOTAL,), jnp.float32, 1.0 / 50.0, 1.0 / 30.0)
    slow_rate = 0.2 / TOKEN_TOTAL * jax.random.uniform(random_key_list[2], (HEAD_TOTAL,), jnp.float32, 0.5, 1.0)
    medium_rate = jax.random.uniform(random_key_list[7], (HEAD_TOTAL,), jnp.float32, 1.2, 2.0) / TOK_DEV
    baseline_decay_rate = jnp.where(fast_flag, fast_rate, jnp.where(medium_flag, medium_rate, slow_rate))
    noisy_inputs = jax.random.uniform(random_key_list[3], (HEAD_TOTAL, TOKEN_TOTAL), jnp.float32, 0.5, 2.0)
    shard_multiplier = jax.random.uniform(random_key_list[4], (HEAD_TOTAL, shard_count), jnp.float32, 0.5, 1.0)
    shard_multiplier = jnp.repeat(shard_multiplier, TOK_DEV, axis=1)
    spike_positions = jax.random.randint(random_key_list[5], (3,), 0, TOKEN_TOTAL)
    spike_token_mask = jnp.any(jnp.arange(TOKEN_TOTAL)[None, :] == spike_positions[:, None], axis=0)
    spike_loss_value = jax.random.uniform(random_key_list[6], (HEAD_TOTAL,), jnp.float32, -0.5, -0.22)
    spike_events = jnp.where(slow_flag[:, None] & spike_token_mask[None, :], spike_loss_value[:, None], 0.0)
    baseline = -baseline_decay_rate[:, None] * noisy_inputs * shard_multiplier + spike_events
    strong_pick = jax.random.randint(random_key_list[8], (HEAD_TOTAL, shard_count), 0, 4) == 0
    forced_shard = jax.random.randint(random_key_list[9], (HEAD_TOTAL,), 0, shard_count)
    strong_pick = strong_pick | (jnp.arange(shard_count)[None, :] == forced_shard[:, None])
    strong_tokens = jnp.repeat(strong_pick, TOK_DEV, axis=1) & fast_flag[:, None]
    strong_value = -jax.random.uniform(random_key_list[10], (HEAD_TOTAL, TOKEN_TOTAL), jnp.float32, 0.3, 0.5)
    return jnp.where(strong_tokens, strong_value, baseline).astype(jnp.float32)


def levels(rng, dims, cuts, least, high):
    level = 1.0
    for position, parts in cuts:
        steps = jax.random.uniform(jax.random.fold_in(jax.random.fold_in(rng, 6), position), (parts,), jnp.float32, least / len(cuts), high / len(cuts))
        level = level * jnp.repeat(jnp.exp(steps), dims[position] // parts).reshape((-1,) + (1,) * (len(dims) - 1 - position))
    return level


def bell_draw(key, dims, scale, bound, cuts=(), held_as=jnp.bfloat16):
    array = jax.random.normal(key, dims, jnp.float32) * scale
    if len(cuts) > 0:
        array = levels(key, dims, cuts, -0.22, 0.18) * array
    return jnp.clip(array, min=-bound, max=bound).astype(held_as)


def setup_inputs(seed: int = 0) -> dict:
    key_of = jax.random.split(jax.random.key(seed), 7)
    inputs = bell_draw(key_of[0], (TOKEN_TOTAL, HEAD_TOTAL * HEAD_DIM), 0.5, 3.0, ((0, 64), (1, 4)), jnp.float32)
    log_decay = draw_log_decay(jax.random.fold_in(key_of[6], 71), 0)
    b_proj = bell_draw(key_of[2], (TOKEN_TOTAL, D_STATE), 0.09, 0.5, ((0, 64),), jnp.float32)
    c_proj = bell_draw(key_of[3], (TOKEN_TOTAL, D_STATE), 0.09, 0.5, ((0, 64),), jnp.float32)
    entry_states = bell_draw(key_of[4], (SHARDS, HEAD_TOTAL, HEAD_DIM, D_STATE), 2.0, 12.0, ((0, 64), (1, 4)), jnp.float32)
    out_grad = bell_draw(key_of[5], (TOKEN_TOTAL, HEAD_TOTAL * HEAD_DIM), 0.5, 3.0, ((0, 64), (1, 4)), jnp.float32)
    return {"inputs": inputs, "log_decay": log_decay, "b_proj": b_proj, "c_proj": c_proj, "entry_states": entry_states, "out_grad": out_grad}


def advance(inputs, log_decay, b_proj, c_proj, entry):
    head_count = log_decay.shape[0]
    tok_count = inputs.shape[0]
    head_width = inputs.shape[1] // head_count
    block_count = tok_count // BLOCK
    highest = lax.Precision.HIGHEST
    blocked_in = inputs.reshape(block_count, BLOCK, head_count, head_width)
    rates = log_decay.reshape(head_count, block_count, BLOCK).transpose(1, 0, 2)
    b_blocks = b_proj.reshape(block_count, BLOCK, -1)
    c_blocks = c_proj.reshape(block_count, BLOCK, -1)
    cumulative = jnp.cumsum(rates, axis=2)
    causal = jnp.arange(BLOCK)[:, None] >= jnp.arange(BLOCK)[None, :]
    log_gap = cumulative[:, :, :, None] - cumulative[:, :, None, :]
    decay_table = jnp.where(causal, jnp.exp(jnp.where(causal, log_gap, 0.0)), 0.0)
    scores = jnp.einsum('cln,csn->cls', c_blocks, b_blocks, precision=highest)
    mixing = decay_table * scores[:, None]
    inner_out = jnp.einsum('chls,cshp->clhp', mixing, blocked_in, precision=highest)
    tail_decay = jnp.exp(cumulative[:, :, -1:] - cumulative)
    block_states = jnp.einsum('chs,cshp,csn->chpn', tail_decay, blocked_in, b_blocks, precision=highest)
    totals = jnp.exp(cumulative[:, :, -1])
    current = entry
    entering = []
    for block_index in range(block_count):
        entering.append(current)
        current = totals[block_index][:, None, None] * current + block_states[block_index]
    stacked = jnp.stack(entering)
    outer_out = jnp.einsum('cln,chpn,chl->clhp', c_blocks, stacked, jnp.exp(cumulative), precision=highest)
    return ((inner_out + outer_out).reshape(tok_count, head_count * head_width), current)

def reference(inputs, log_decay, b_proj, c_proj, entry_states, out_grad):
    head_count = log_decay.shape[0]
    shard_in = inputs.reshape(SHARDS, TOK_DEV, -1)
    shard_rates = log_decay.reshape(head_count, SHARDS, TOK_DEV).transpose(1, 0, 2)
    shard_b = b_proj.reshape(SHARDS, TOK_DEV, -1)
    shard_c = c_proj.reshape(SHARDS, TOK_DEV, -1)
    shard_grad = out_grad.reshape(SHARDS, TOK_DEV, -1)

    def backward(later, pieces):
        piece_in, piece_rates, piece_b, piece_c, piece_entry, piece_grad = pieces
        unused, pullback = jax.vjp(advance, piece_in, piece_rates, piece_b, piece_c, piece_entry)
        grads = pullback((piece_grad, later))
        return (grads[4], grads)
    start = jnp.zeros(entry_states.shape[1:], jnp.float32)
    unused, collected = lax.scan(backward, start, (shard_in, shard_rates, shard_b, shard_c, entry_states, shard_grad), reverse=True)
    grad_in, grad_rates, grad_b, grad_c, grad_entry = collected
    d_inputs = grad_in.reshape(TOKEN_TOTAL, -1)
    d_log_decay = grad_rates.transpose(1, 0, 2).reshape(head_count, TOKEN_TOTAL)
    return (d_inputs, d_log_decay, grad_b.reshape(TOKEN_TOTAL, -1), grad_c.reshape(TOKEN_TOTAL, -1), grad_entry)
```

```python
import functools

import jax
import jax.numpy as jnp
from jax import lax
from jax.experimental import pallas as pl
from jax.experimental.pallas import tpu as pltpu
from jax.sharding import PartitionSpec as P

F32 = jnp.float32
BF16 = jnp.bfloat16
MESH = pl.DeviceIdType.MESH
TOK = 512
HEADS = 20
WIDTH = 64
STATE = 128
ROWS = HEADS * WIDTH
PAIRS = HEADS // 2
TILE = 128
LOG2E = 1.4426950408889634
ZN = 8
XN = 4
HN = 4
HALF = STATE // 2
SLICE = HALF // ZN


def split(v):
    hi = v.astype(BF16)
    return hi, (v - hi.astype(F32)).astype(BF16)


def split3(v):
    hi = v.astype(BF16)
    rest = v - hi.astype(F32)
    mid = rest.astype(BF16)
    return hi, mid, (rest - mid.astype(F32)).astype(BF16)


def nn(a, b):
    return lax.dot_general(a, b, (((1,), (0,)), ((), ())), preferred_element_type=F32)


def nt(a, b):
    return lax.dot_general(a, b, (((1,), (1,)), ((), ())), preferred_element_type=F32)


def nn3(a, b):
    a_hi, a_lo = a
    b_hi, b_lo = b
    width = b_hi.shape[1]
    both = nn(a_hi, jnp.concatenate([b_hi, b_lo], axis=1))
    return both[:, :width] + both[:, width:] + nn(a_lo, b_hi)


def nt3(a, b):
    a_hi, a_lo = a
    b_hi, b_lo = b
    return nt(a_hi, b_hi) + nt(a_hi, b_lo) + nt(a_lo, b_hi)


def iota(shape, dim):
    return lax.broadcasted_iota(jnp.int32, shape, dim)


def prefix_sums(value, strict):
    rows = value.shape[0]
    a, b = iota((TILE, TILE), 0), iota((TILE, TILE), 1)
    upper = jnp.where(a < b if strict else a <= b, 1.0, 0.0).astype(BF16)
    tiles = []
    base = jnp.zeros((rows, 1), F32)
    for j in range(TOK // TILE):
        part = value[:, j * TILE : (j + 1) * TILE]
        hi, mid, lo = split3(part)
        inner = nn(hi, upper) + nn(mid, upper) + nn(lo, upper)
        tiles.append(inner + base)
        last = tiles[-1][:, TILE - 1 : TILE]
        base = last + part[:, TILE - 1 : TILE] if strict else last
    return jnp.concatenate(tiles, axis=1)


def pair_picker():
    row, lane = iota((8, TILE), 0), iota((8, TILE), 1)
    low = (row == 0) & (lane < WIDTH)
    high = (row == 1) & (lane >= WIDTH)
    return jnp.where(low | high, 1.0, 0.0).astype(BF16)


def local_kernel(
    x_ref, ld_ref, b_ref, c_ref, s0_ref, dy_ref,
    gt_ref, a_ref, l3_ref, dx_ref, txh_ref, txl_ref, tail_ref, v_ref, db_ref, dc_ref,
    ld32, lx, lrow, cbt, et, eh, el,
):
    first = iota((1, TILE), 1) < WIDTH
    ld32[...] = jnp.zeros_like(ld32)
    ld32[0:HEADS, :] = ld_ref[...] * LOG2E
    cum = prefix_sums(ld32[...], False)
    for h in range(HEADS):
        lrow[h] = cum[h : h + 1, :]
    hi, mid, lo = split3(cum)
    stack = jnp.concatenate(
        [hi.astype(F32), mid.astype(F32), lo.astype(F32), jnp.zeros_like(cum)], axis=0
    )
    columns = stack.T
    l3_ref[...] = columns[TOK - 1 : TOK, :]
    columns = columns.astype(BF16)
    spread = jnp.where(
        (iota((TILE, HEADS * TILE), 0) & 31) == (iota((TILE, HEADS * TILE), 1) >> 7), 1.0, 0.0
    ).astype(BF16)
    for k in range(HEADS // 4):
        part = slice(k * 4 * TILE, (k + 1) * 4 * TILE)
        lx[:, part] = nn(columns, spread[:, part])

    c_pair = split(c_ref[...])
    ct_pair = split(c_ref[...].T)
    b_pair = split(b_ref[...])

    def start(p, carry):
        tile = pl.ds(pl.multiple_of(p * TILE, TILE), TILE)
        la = lx[:, pl.ds(pl.multiple_of(p * 2 * TILE, TILE), TILE)]
        lb = lx[:, pl.ds(pl.multiple_of(p * 2 * TILE + TILE, TILE), TILE)]
        both = jnp.where(first, la, lb)
        e_pair = split(jnp.exp2(both) * dy_ref[:, tile])
        eh[:, tile] = e_pair[0]
        el[:, tile] = e_pair[1]
        gt_ref[:, tile] = nn3(ct_pair, e_pair)
        end = both[TOK - 1 : TOK, :]
        a_ref[:, tile] = jnp.exp2(end)
        tail = jnp.exp2(end - both)
        tail_ref[:, tile] = tail
        tx = split(tail * x_ref[:, tile])
        txh_ref[:, tile] = tx[0]
        txl_ref[:, tile] = tx[1]
        return carry

    lax.fori_loop(0, PAIRS, start, 0)

    causal = iota((TOK, TOK), 0) <= iota((TOK, TOK), 1)
    cbt[...] = jnp.where(causal, nt3(b_pair, c_pair), 0.0)
    et[...] = jnp.zeros_like(et)
    picker = pair_picker()
    sub = iota((8, TOK), 0)

    def inner(p, carry):
        tile = pl.ds(pl.multiple_of(p * TILE, TILE), TILE)
        x, dy = x_ref[:, tile], dy_ref[:, tile]
        xh, xl = split(x)
        dyh, dyl = split(dy)
        xh_f, dyh_f = xh.astype(F32), dyh.astype(F32)
        x_turn = pltpu.roll(xl.astype(F32), WIDTH, 1)
        dy_turn = pltpu.roll(dyh_f, WIDTH, 1)
        dyl_f = dyl.astype(F32)
        zero = jnp.zeros_like(x)
        dycat = jnp.concatenate([dyh, dyl], axis=1)
        left, right, turn = [], [], []
        for k in range(2):
            here = first if k == 0 else jnp.logical_not(first)
            left.append(
                jnp.concatenate(
                    [jnp.where(here, xh_f, x_turn), jnp.where(here, xh_f, zero)], axis=1
                ).astype(BF16)
            )
            right.append(
                jnp.concatenate(
                    [jnp.where(here, dyh_f, dy_turn), jnp.where(here, dyl_f, zero)], axis=1
                ).astype(BF16)
            )
        z = [[jnp.zeros((1, TILE), F32) for j in range(4)] for k in range(2)]
        for i in range(4):
            r = i * TILE
            mix = cbt[r : r + TILE, r:]
            outs = []
            gained = et[r : r + TILE, r:]
            for k in range(2):
                grad = nt(left[k][r : r + TILE], right[k][r:])
                column = lx[r : r + TILE, pl.ds(pl.multiple_of((2 * p + k) * TILE, TILE), TILE)]
                row = lrow[2 * p + k][:, r:]
                decay = []
                for j in range(4 - i):
                    gap = row[:, j * TILE : (j + 1) * TILE] - column
                    decay.append(jnp.exp2(jnp.minimum(gap, 0.0) if j == 0 else gap))
                decay = jnp.concatenate(decay, axis=1)
                weight = decay * mix
                gained = gained + decay * grad
                sums = jnp.sum(weight * grad, axis=0, keepdims=True)
                for j in range(4 - i):
                    z[k][i + j] = z[k][i + j] + sums[:, j * TILE : (j + 1) * TILE]
                wh, wl = split(weight)
                wide = nn(wh, dycat[r:])
                outs.append(wide[:, :TILE] + wide[:, TILE:] + nn(wl, dyh[r:]))
            et[r : r + TILE, r:] = gained
            dx_ref[r : r + TILE, tile] = jnp.where(first, outs[0], outs[1])
        rows = pl.ds(pl.multiple_of(p * TILE, TILE), TILE)
        entering = nt3(c_pair, split(s0_ref[rows, :]))
        e = eh[:, tile].astype(F32) + el[:, tile].astype(F32)
        vh, vl = split(x * dx_ref[:, tile] - e * entering)
        za, zb = jnp.concatenate(z[0], axis=1), jnp.concatenate(z[1], axis=1)
        v_ref[p] = (
            nt(picker, vh)
            + nt(picker, vl)
            - jnp.where(sub == 0, za, jnp.where(sub == 1, zb, 0.0))
        )
        return carry

    lax.fori_loop(0, PAIRS, inner, 0)

    table = jnp.where(causal, et[...], 0.0)
    db_ref[...] = nn3(split(table), c_pair)
    s_pair = split(s0_ref[...])
    dc_ref[...] = nn3(split(table.T), b_pair) + nn3((eh[...], el[...]), s_pair)


def run_local(x, ld, b, c, s0, dy):
    vm = pl.BlockSpec(memory_space=pltpu.VMEM)
    shape = jax.ShapeDtypeStruct
    return pl.pallas_call(
        local_kernel,
        out_shape=(
            shape((STATE, ROWS), F32),
            shape((1, ROWS), F32),
            shape((1, TILE), F32),
            shape((TOK, ROWS), F32),
            shape((TOK, ROWS), BF16),
            shape((TOK, ROWS), BF16),
            shape((TOK, ROWS), F32),
            shape((PAIRS, 8, TOK), F32),
            shape((TOK, STATE), F32),
            shape((TOK, STATE), F32),
        ),
        in_specs=[vm] * 6,
        out_specs=(vm,) * 10,
        scratch_shapes=[
            pltpu.VMEM((32, TOK), F32),
            pltpu.VMEM((TOK, HEADS * TILE), F32),
            pltpu.VMEM((HEADS, 1, TOK), F32),
            pltpu.VMEM((TOK, TOK), F32),
            pltpu.VMEM((TOK, TOK), F32),
            pltpu.VMEM((TOK, ROWS), BF16),
            pltpu.VMEM((TOK, ROWS), BF16),
        ],
        compiler_params=pltpu.CompilerParams(vmem_limit_bytes=60 * 1024 * 1024),
        name="local",
    )(x, ld, b, c, s0, dy)


def scan_kernel(
    gt_ref, l3_ref, out_ref,
    pg, pl3, chip, chip_l3, g1, zbuf, zl3, inside, xg, xl, lbuf, back, other,
    pair_s, pair_r, z_s, z_r, x_s, x_r, b_s, b_r,
):
    me, hd = lax.axis_index("seq"), lax.axis_index("head")
    core = lax.rem(me, 2)
    z = lax.rem(me // 2, ZN)
    x = me // (2 * ZN)

    def peer(px, pz, pc):
        return (px * 2 * ZN + pz * 2 + pc, hd)

    mate = peer(x, z, 1 - core)
    z_peers = [lax.rem(z + d, ZN) for d in range(1, ZN)]
    x_peers = [lax.rem(x + d, XN) for d in range(1, XN)]
    barrier = pltpu.get_barrier_semaphore()
    everyone = [mate] + [peer(x, q, core) for q in z_peers] + [peer(q, z, core) for q in x_peers]
    for device in everyone:
        pl.semaphore_signal(barrier, inc=1, device_id=device, device_id_type=MESH)
    pl.semaphore_wait(barrier, len(everyone))

    def send(src, dst, s, r, device):
        copy = pltpu.make_async_remote_copy(
            src_ref=src, dst_ref=dst, send_sem=s, recv_sem=r, device_id=device, device_id_type=MESH
        )
        copy.start()
        return copy

    away = pl.ds(pl.multiple_of((1 - core) * HALF, HALF), HALF)
    mine = pl.ds(pl.multiple_of(core * HALF, HALF), HALF)
    c0 = send(gt_ref.at[away], pg, pair_s.at[0], pair_r.at[0], mate)
    c1 = send(l3_ref, pl3, pair_s.at[1], pair_r.at[1], mate)
    spread = jnp.where(
        (iota((TILE, ROWS), 0) & 31) == (iota((TILE, ROWS), 1) >> 6), 1.0, 0.0
    ).astype(BF16)
    even = core == 0
    c1.wait()
    own_l3, mate_l3 = l3_ref[...], pl3[...]
    l0 = jnp.where(even, own_l3, mate_l3)
    l1 = jnp.where(even, mate_l3, own_l3)
    chip_l3[0] = l0
    chip_l3[1] = l1
    pair_logs = nn(jnp.concatenate([l0, l1], axis=0).astype(BF16), spread)
    a0, a1 = jnp.exp2(pair_logs[0:1]), jnp.exp2(pair_logs[1:2])
    c0.wait()
    for j in range(ZN):
        rows = pl.ds(pl.multiple_of(core * HALF + j * SLICE, SLICE), SLICE)
        part, mate_part = gt_ref[rows, :], pg[j * SLICE : (j + 1) * SLICE, :]
        later = jnp.where(even, mate_part, part)
        g1[j] = later
        chip[j] = jnp.where(even, part, mate_part) + a0 * later
    copies = []
    for q, d in zip(z_peers, range(ZN - 1)):
        device = peer(x, q, core)
        copies.append(send(chip_l3, zl3.at[z], z_s.at[0, d], z_r.at[0, d], device))
        copies.append(send(chip.at[q], zbuf.at[z], z_s.at[1, d], z_r.at[1, d], device))
    zbuf[z] = chip[z]
    zl3[z] = chip_l3[...]
    for copy in copies:
        copy.wait()
    logs = [nn(jnp.concatenate([zl3[j, 0], zl3[j, 1]], axis=0).astype(BF16), spread) for j in range(ZN)]
    logs = [v[0:1] + v[1:2] for v in logs]
    state = jnp.zeros((SLICE, ROWS), F32)
    log = jnp.zeros((1, ROWS), F32)
    factor = [None] * ZN
    for j in reversed(range(ZN)):
        inside[j] = state
        factor[j] = jnp.exp2(log)
        state = zbuf[j] + jnp.exp2(logs[j]) * state
        log = log + logs[j]
    xg[x] = state
    xl[x] = jnp.exp2(log)
    copies = []
    for q, d in zip(x_peers, range(XN - 1)):
        device = peer(q, z, core)
        copies.append(send(xl.at[x], xl.at[x], x_s.at[0, d], x_r.at[0, d], device))
        copies.append(send(xg.at[x], xg.at[x], x_s.at[1, d], x_r.at[1, d], device))
    for copy in copies:
        copy.wait()
    carry = jnp.zeros((SLICE, ROWS), F32)
    for q in reversed(range(1, XN)):
        carry = jnp.where(q > x, xg[q] + xl[q] * carry, carry)
    for j in range(ZN):
        lbuf[j] = inside[j] + factor[j] * carry
    copies = []
    for q, d in zip(z_peers, range(ZN - 1)):
        copies.append(send(lbuf.at[q], back.at[z], b_s.at[d], b_r.at[d], peer(x, q, core)))
    back[z] = lbuf[z]
    for copy in copies:
        copy.wait()
    for j in range(ZN):
        late = back[j]
        early = g1[j] + a1 * late
        rows = pl.ds(pl.multiple_of(core * HALF + j * SLICE, SLICE), SLICE)
        out_ref[rows, :] = jnp.where(even, early, late)
        other[j * SLICE : (j + 1) * SLICE, :] = jnp.where(even, late, early)
    c2 = send(other, out_ref.at[mine], pair_s.at[2], pair_r.at[2], mate)
    c2.wait()


def run_scan(gt, l3):
    vm = pl.BlockSpec(memory_space=pltpu.VMEM)
    dma = pltpu.SemaphoreType.DMA
    slab = pltpu.VMEM((ZN, SLICE, ROWS), F32)
    return pl.pallas_call(
        scan_kernel,
        out_shape=jax.ShapeDtypeStruct((STATE, ROWS), F32),
        in_specs=[vm, vm],
        out_specs=vm,
        scratch_shapes=[
            pltpu.VMEM((HALF, ROWS), F32),
            pltpu.VMEM((1, TILE), F32),
            slab,
            pltpu.VMEM((2, 1, TILE), F32),
            slab,
            slab,
            pltpu.VMEM((ZN, 2, 1, TILE), F32),
            slab,
            pltpu.VMEM((XN, SLICE, ROWS), F32),
            pltpu.VMEM((XN, 1, ROWS), F32),
            slab,
            slab,
            pltpu.VMEM((HALF, ROWS), F32),
            dma((3,)), dma((3,)),
            dma((2, ZN - 1)), dma((2, ZN - 1)),
            dma((2, XN - 1)), dma((2, XN - 1)),
            dma((ZN - 1,)), dma((ZN - 1,)),
        ],
        compiler_params=pltpu.CompilerParams(
            collective_id=0, has_side_effects=True, vmem_limit_bytes=32 * 1024 * 1024
        ),
        name="scan",
    )(gt, l3)


def final_kernel(
    lat_ref, txh_ref, txl_ref, tail_ref, dxl_ref, gt_ref, a_ref, s0_ref, b_ref, v_ref, dbl_ref, dc_ref,
    dx_ref, dld_ref, sum_ref, eg_ref,
    lh, ll, w, g1, own, got,
    r_s, r_r, g_s, g_r,
):
    me, hd = lax.axis_index("seq"), lax.axis_index("head")
    peers = [lax.rem(hd + d, HN) for d in range(1, HN)]
    barrier = pltpu.get_barrier_semaphore()
    for q in peers:
        pl.semaphore_signal(barrier, inc=1, device_id=(me, q), device_id_type=MESH)
    pl.semaphore_wait(barrier, HN - 1)

    hi, lo = split(lat_ref[...])
    lh[...] = hi
    ll[...] = lo
    db = nt3((txh_ref[...], txl_ref[...]), (hi, lo)) + dbl_ref[...]
    part = TOK // HN
    for q in range(HN):
        rows = slice(q * part, (q + 1) * part)
        own[q, :, 0:STATE] = db[rows]
        own[q, :, STATE:] = dc_ref[rows, :]
    copies = []
    for q, d in zip(peers, range(HN - 1)):
        copy = pltpu.make_async_remote_copy(
            src_ref=own.at[q], dst_ref=got.at[d], send_sem=r_s.at[d], recv_sem=r_r.at[d],
            device_id=(me, q), device_id_type=MESH,
        )
        copy.start()
        copies.append(copy)

    b_pair = split(b_ref[...])
    picker = pair_picker()
    sub = iota((8, TILE), 0)

    def correct(p, carry):
        tile = pl.ds(pl.multiple_of(p * TILE, TILE), TILE)
        pair = (lh[:, tile], ll[:, tile])
        raw = nn3(b_pair, pair)
        dx_ref[:, tile] = dxl_ref[:, tile] + tail_ref[:, tile] * raw
        tx = txh_ref[:, tile].astype(F32) + txl_ref[:, tile].astype(F32)
        vh, vl = split(tx * raw)
        w[pl.ds(pl.multiple_of(p * 8, 8), 8), :] = v_ref[p] + nt(picker, vh) + nt(picker, vl)
        eg = (a_ref[:, tile] * lat_ref[:, tile] + gt_ref[:, tile]).T
        rows = pl.ds(pl.multiple_of(p * TILE, TILE), TILE)
        eg_ref[rows, :] = eg
        product = eg * s0_ref[rows, :]
        one = jnp.sum(jnp.sum(product[:WIDTH], axis=0, keepdims=True), axis=1, keepdims=True)
        two = jnp.sum(jnp.sum(product[WIDTH:], axis=0, keepdims=True), axis=1, keepdims=True)
        g1[pl.ds(pl.multiple_of(p * 8, 8), 8), :] = jnp.where(
            sub == 0, one, jnp.where(sub == 1, two, 0.0)
        )
        return carry

    lax.fori_loop(0, PAIRS, correct, 0)
    rates = prefix_sums(w[...], True) + g1[:, 0:1]
    for h in range(HEADS):
        k = (h // 2) * 8 + h % 2
        dld_ref[h : h + 1, :] = rates[k : k + 1, :]

    for copy in copies:
        copy.wait()
    here = pl.ds(pl.multiple_of(hd * part, part), part)
    sum_ref[here, :] = own[hd] + got[0] + got[1] + got[2]
    copies = []
    for q, d in zip(peers, range(HN - 1)):
        copy = pltpu.make_async_remote_copy(
            src_ref=sum_ref.at[here], dst_ref=sum_ref.at[here], send_sem=g_s.at[d], recv_sem=g_r.at[d],
            device_id=(me, q), device_id_type=MESH,
        )
        copy.start()
        copies.append(copy)
    for copy in copies:
        copy.wait()


def run_final(lat, txh, txl, tail, dxl, gt, a, s0, b, v, dbl, dc):
    vm = pl.BlockSpec(memory_space=pltpu.VMEM)
    dma = pltpu.SemaphoreType.DMA
    shape = jax.ShapeDtypeStruct
    return pl.pallas_call(
        final_kernel,
        out_shape=(
            shape((TOK, ROWS), F32),
            shape((HEADS, TOK), F32),
            shape((TOK, 2 * STATE), F32),
            shape((ROWS, STATE), F32),
        ),
        in_specs=[vm] * 12,
        out_specs=(vm,) * 4,
        scratch_shapes=[
            pltpu.VMEM((STATE, ROWS), BF16),
            pltpu.VMEM((STATE, ROWS), BF16),
            pltpu.VMEM((PAIRS * 8, TOK), F32),
            pltpu.VMEM((PAIRS * 8, TILE), F32),
            pltpu.VMEM((HN, TOK // HN, 2 * STATE), F32),
            pltpu.VMEM((HN - 1, TOK // HN, 2 * STATE), F32),
            dma((HN - 1,)), dma((HN - 1,)), dma((HN - 1,)), dma((HN - 1,)),
        ],
        compiler_params=pltpu.CompilerParams(
            collective_id=1, has_side_effects=True, vmem_limit_bytes=60 * 1024 * 1024
        ),
        name="final",
    )(lat, txh, txl, tail, dxl, gt, a, s0, b, v, dbl, dc)


def per_device(inputs, log_decay, b_proj, c_proj, entry_states, out_grad):
    s0 = entry_states.reshape(ROWS, STATE)
    gt, a, l3, dxl, txh, txl, tail, v, dbl, dc = run_local(
        inputs, log_decay, b_proj, c_proj, s0, out_grad
    )
    lat = run_scan(gt, l3)
    dx, dld, total, eg = run_final(lat, txh, txl, tail, dxl, gt, a, s0, b_proj, v, dbl, dc)
    return (dx, dld, total[:, :STATE], total[:, STATE:], eg.reshape(1, HEADS, WIDTH, STATE))


def solution(mesh):
    return jax.shard_map(
        per_device,
        mesh=mesh,
        in_specs=(
            P("seq", "head"),
            P("head", "seq"),
            P("seq", None),
            P("seq", None),
            P("seq", "head", None, None),
            P("seq", "head"),
        ),
        out_specs=(
            P("seq", "head"),
            P("head", "seq"),
            P("seq", None),
            P("seq", None),
            P("seq", "head", None, None),
        ),
        check_vma=False,
    )
```

```python
import functools

import jax
import jax.numpy as jnp
from jax import lax
from jax.experimental import pallas as pl
from jax.experimental.pallas import tpu as pltpu
from jax.sharding import PartitionSpec as P

F32 = jnp.float32
BF16 = jnp.bfloat16
MESH = pl.DeviceIdType.MESH
TOK = 512
HEADS = 20
WIDTH = 64
STATE = 128
ROWS = HEADS * WIDTH
PAIRS = HEADS // 2
TILE = 128
LOG2E = 1.4426950408889634
ZN = 8
XN = 4
HN = 4
HALF = STATE // 2
SLICE = HALF // ZN
CUT_Z = 4
CUT_X = 6
CUT_Y = 5
VMEM_LIMIT = 58 * 1024 * 1024
OUT = pltpu.VMEM


def split(v):
    hi = v.astype(BF16)
    return hi, (v - hi.astype(F32)).astype(BF16)


def split3(v):
    hi = v.astype(BF16)
    rest = v - hi.astype(F32)
    mid = rest.astype(BF16)
    return hi, mid, (rest - mid.astype(F32)).astype(BF16)


def nn(a, b):
    return lax.dot_general(a, b, (((1,), (0,)), ((), ())), preferred_element_type=F32)


def nt(a, b):
    return lax.dot_general(a, b, (((1,), (1,)), ((), ())), preferred_element_type=F32)


def nn3(a, b):
    a_hi, a_lo = a
    b_hi, b_lo = b
    width = b_hi.shape[1]
    both = nn(a_hi, jnp.concatenate([b_hi, b_lo], axis=1))
    return both[:, :width] + both[:, width:] + nn(a_lo, b_hi)


def nt3(a, b):
    a_hi, a_lo = a
    b_hi, b_lo = b
    return nt(a_hi, b_hi) + nt(a_hi, b_lo) + nt(a_lo, b_hi)


def iota(shape, dim):
    return lax.broadcasted_iota(jnp.int32, shape, dim)


def prefix_sums(value, strict):
    rows = value.shape[0]
    a, b = iota((TILE, TILE), 0), iota((TILE, TILE), 1)
    upper = jnp.where(a < b if strict else a <= b, 1.0, 0.0).astype(BF16)
    tiles = []
    base = jnp.zeros((rows, 1), F32)
    for j in range(TOK // TILE):
        part = value[:, j * TILE : (j + 1) * TILE]
        hi, mid, lo = split3(part)
        inner = nn(hi, upper) + nn(mid, upper) + nn(lo, upper)
        tiles.append(inner + base)
        last = tiles[-1][:, TILE - 1 : TILE]
        base = last + part[:, TILE - 1 : TILE] if strict else last
    return jnp.concatenate(tiles, axis=1)


def pair_picker():
    row, lane = iota((8, TILE), 0), iota((8, TILE), 1)
    low = (row == 0) & (lane < WIDTH)
    high = (row == 1) & (lane >= WIDTH)
    return jnp.where(low | high, 1.0, 0.0).astype(BF16)


def main_kernel(
    x_hbm, ld_ref, b_ref, c_ref, s0_hbm, dy_hbm,
    dx_ref, dld_ref, db_ref, dc_ref, eg_ref,
    x_ref, s0_ref, dy_ref, gt_ref, a_ref, txh, txl, tail_ref, v_ref, dbl,
    ld32, lx, lrow, cbt, et, eh, el,
    l3, pg, pl3, chip, chip_l3, g1, zbuf, zl3, inside, fac, xg, xl, lbuf, back, other, lat,
    lh, ll, w, first_g, own_c, got_c, own_b, got_b,
    in_s, pair_s, pair_r, z_s, z_r, x_s, x_r, b_s, b_r, y_s, y_r,
):
    me, hd = lax.axis_index("seq"), lax.axis_index("head")
    core = lax.rem(me, 2)
    z = lax.rem(me // 2, ZN)
    x = me // (2 * ZN)
    even = core == 0

    def peer(px, pz, pc):
        return (px * 2 * ZN + pz * 2 + pc, hd)

    mate = peer(x, z, 1 - core)
    z_peers = [lax.rem(z + d, ZN) for d in range(1, ZN)]
    x_peers = [lax.rem(x + d, XN) for d in range(1, XN)]
    y_peers = [lax.rem(hd + d, HN) for d in range(1, HN)]
    barrier = pltpu.get_barrier_semaphore()
    everyone = (
        [mate]
        + [peer(x, q, core) for q in z_peers]
        + [peer(q, z, core) for q in x_peers]
        + [(me, q) for q in y_peers]
    )
    for device in everyone:
        pl.semaphore_signal(barrier, inc=1, device_id=device, device_id_type=MESH)
    loads = [
        pltpu.make_async_copy(dy_hbm, dy_ref, in_s.at[0]),
        pltpu.make_async_copy(x_hbm, x_ref, in_s.at[1]),
        pltpu.make_async_copy(s0_hbm, s0_ref, in_s.at[2]),
    ]
    for load in loads:
        load.start()

    def send(src, dst, s, r, device):
        copy = pltpu.make_async_remote_copy(
            src_ref=src, dst_ref=dst, send_sem=s, recv_sem=r, device_id=device, device_id_type=MESH
        )
        copy.start()
        return copy

    first = iota((1, TILE), 1) < WIDTH
    ld32[...] = jnp.zeros_like(ld32)
    ld32[0:HEADS, :] = ld_ref[...] * LOG2E
    cum = prefix_sums(ld32[...], False)
    for h in range(HEADS):
        lrow[h] = cum[h : h + 1, :]
    hi, mid, lo = split3(cum)
    stack = jnp.concatenate(
        [hi.astype(F32), mid.astype(F32), lo.astype(F32), jnp.zeros_like(cum)], axis=0
    )
    columns = stack.T
    l3[...] = columns[TOK - 1 : TOK, :]
    columns = columns.astype(BF16)
    wide = (TILE, HEADS * TILE)
    spread = jnp.where((iota(wide, 0) & 31) == (iota(wide, 1) >> 7), 1.0, 0.0).astype(BF16)
    for k in range(HEADS // 4):
        part = slice(k * 4 * TILE, (k + 1) * 4 * TILE)
        lx[:, part] = nn(columns, spread[:, part])
    ct_pair = split(c_ref[...].T)
    loads[0].wait()

    def tile_of(p):
        return pl.ds(pl.multiple_of(p * TILE, TILE), TILE)

    def logs_of(p):
        la = lx[:, pl.ds(pl.multiple_of(p * 2 * TILE, TILE), TILE)]
        lb = lx[:, pl.ds(pl.multiple_of(p * 2 * TILE + TILE, TILE), TILE)]
        return jnp.where(first, la, lb)

    def start(p, carry):
        tile = tile_of(p)
        both = logs_of(p)
        e_pair = split(jnp.exp2(both) * dy_ref[:, tile])
        eh[:, tile] = e_pair[0]
        el[:, tile] = e_pair[1]
        gt_ref[:, tile] = nn3(ct_pair, e_pair)
        return carry

    lax.fori_loop(0, PAIRS, start, 0)

    pl.semaphore_wait(barrier, len(everyone))
    away = pl.ds(pl.multiple_of((1 - core) * HALF, HALF), HALF)
    mine = pl.ds(pl.multiple_of(core * HALF, HALF), HALF)
    c1 = send(l3, pl3, pair_s.at[1], pair_r.at[1], mate)
    c0 = send(gt_ref.at[away], pg, pair_s.at[0], pair_r.at[0], mate)

    c_pair = split(c_ref[...])
    b_pair = split(b_ref[...])
    causal = iota((TOK, TOK), 0) <= iota((TOK, TOK), 1)
    cbt[...] = jnp.where(causal, nt3(b_pair, c_pair), 0.0)
    et[...] = jnp.zeros_like(et)

    narrow = (TILE, ROWS)
    spread = jnp.where((iota(narrow, 0) & 31) == (iota(narrow, 1) >> 6), 1.0, 0.0).astype(BF16)
    c1.wait()
    own_l3, mate_l3 = l3[...], pl3[...]
    l0 = jnp.where(even, own_l3, mate_l3)
    l1 = jnp.where(even, mate_l3, own_l3)
    chip_l3[0] = l0
    chip_l3[1] = l1
    pair_logs = nn(jnp.concatenate([l0, l1], axis=0).astype(BF16), spread)
    a0, a1 = jnp.exp2(pair_logs[0:1]), jnp.exp2(pair_logs[1:2])
    a_ref[...] = jnp.where(even, a0, a1)
    c0.wait()
    for j in range(ZN):
        rows = pl.ds(pl.multiple_of(core * HALF + j * SLICE, SLICE), SLICE)
        part, mate_part = gt_ref[rows, :], pg[j * SLICE : (j + 1) * SLICE, :]
        later = jnp.where(even, mate_part, part)
        g1[j] = later
        chip[j] = jnp.where(even, part, mate_part) + a0 * later
    z_copies = []
    for q, d in zip(z_peers, range(ZN - 1)):
        device = peer(x, q, core)
        z_copies.append(send(chip_l3, zl3.at[z], z_s.at[0, d], z_r.at[0, d], device))
        z_copies.append(send(chip.at[q], zbuf.at[z], z_s.at[1, d], z_r.at[1, d], device))
    zbuf[z] = chip[z]
    zl3[z] = chip_l3[...]

    picker = pair_picker()
    sub = iota((8, TOK), 0)

    def inner(p, carry):
        tile = tile_of(p)
        xv, dy = x_ref[:, tile], dy_ref[:, tile]
        both = logs_of(p)
        tail = jnp.exp2(both[TOK - 1 : TOK, :] - both)
        tail_ref[:, tile] = tail
        tx = split(tail * xv)
        txh[:, tile] = tx[0]
        txl[:, tile] = tx[1]
        xh, xlo = split(xv)
        dyh, dyl = split(dy)
        xh_f, dyh_f = xh.astype(F32), dyh.astype(F32)
        x_turn = pltpu.roll(xlo.astype(F32), WIDTH, 1)
        dy_turn = pltpu.roll(dyh_f, WIDTH, 1)
        dyl_f = dyl.astype(F32)
        zero = jnp.zeros_like(xv)
        dycat = jnp.concatenate([dyh, dyl], axis=1)
        left, right = [], []
        for k in range(2):
            here = first if k == 0 else jnp.logical_not(first)
            left.append(
                jnp.concatenate(
                    [jnp.where(here, xh_f, x_turn), jnp.where(here, xh_f, zero)], axis=1
                ).astype(BF16)
            )
            right.append(
                jnp.concatenate(
                    [jnp.where(here, dyh_f, dy_turn), jnp.where(here, dyl_f, zero)], axis=1
                ).astype(BF16)
            )
        zs = [[jnp.zeros((1, TILE), F32) for j in range(4)] for k in range(2)]
        for i in range(4):
            r = i * TILE
            mix = cbt[r : r + TILE, r:]
            outs = []
            gained = et[r : r + TILE, r:]
            for k in range(2):
                grad = nt(left[k][r : r + TILE], right[k][r:])
                column = lx[r : r + TILE, pl.ds(pl.multiple_of((2 * p + k) * TILE, TILE), TILE)]
                row = lrow[2 * p + k][:, r:]
                decay = []
                for j in range(4 - i):
                    gap = row[:, j * TILE : (j + 1) * TILE] - column
                    decay.append(jnp.exp2(jnp.minimum(gap, 0.0) if j == 0 else gap))
                decay = jnp.concatenate(decay, axis=1)
                weight = decay * mix
                gained = gained + decay * grad
                sums = jnp.sum(weight * grad, axis=0, keepdims=True)
                for j in range(4 - i):
                    zs[k][i + j] = zs[k][i + j] + sums[:, j * TILE : (j + 1) * TILE]
                wh, wl = split(weight)
                out = nn(wh, dycat[r:])
                outs.append(out[:, :TILE] + out[:, TILE:] + nn(wl, dyh[r:]))
            et[r : r + TILE, r:] = gained
            dx_ref[r : r + TILE, tile] = jnp.where(first, outs[0], outs[1])
        entering = nt3(c_pair, split(s0_ref[tile, :]))
        e = eh[:, tile].astype(F32) + el[:, tile].astype(F32)
        vh, vl = split(xv * dx_ref[:, tile] - e * entering)
        za, zb = jnp.concatenate(zs[0], axis=1), jnp.concatenate(zs[1], axis=1)
        v_ref[p] = (
            nt(picker, vh)
            + nt(picker, vl)
            - jnp.where(sub == 0, za, jnp.where(sub == 1, zb, 0.0))
        )
        return carry

    loads[1].wait()
    loads[2].wait()
    lax.fori_loop(0, CUT_Z, inner, 0)

    for copy in z_copies:
        copy.wait()
    logs = [nn(jnp.concatenate([zl3[j, 0], zl3[j, 1]], axis=0).astype(BF16), spread) for j in range(ZN)]
    logs = [v[0:1] + v[1:2] for v in logs]
    state = jnp.zeros((SLICE, ROWS), F32)
    log = jnp.zeros((1, ROWS), F32)
    for j in reversed(range(ZN)):
        inside[j] = state
        fac[j] = jnp.exp2(log)
        state = zbuf[j] + jnp.exp2(logs[j]) * state
        log = log + logs[j]
    xg[x] = state
    xl[x] = jnp.exp2(log)
    x_copies = []
    for q, d in zip(x_peers, range(XN - 1)):
        device = peer(q, z, core)
        x_copies.append(send(xl.at[x], xl.at[x], x_s.at[0, d], x_r.at[0, d], device))
        x_copies.append(send(xg.at[x], xg.at[x], x_s.at[1, d], x_r.at[1, d], device))

    lax.fori_loop(CUT_Z, CUT_X, inner, 0)

    for copy in x_copies:
        copy.wait()
    entering = jnp.zeros((SLICE, ROWS), F32)
    for q in reversed(range(1, XN)):
        entering = jnp.where(q > x, xg[q] + xl[q] * entering, entering)
    for j in range(ZN):
        lbuf[j] = inside[j] + fac[j] * entering
    b_copies = []
    for q, d in zip(z_peers, range(ZN - 1)):
        b_copies.append(send(lbuf.at[q], back.at[z], b_s.at[d], b_r.at[d], peer(x, q, core)))
    back[z] = lbuf[z]

    lax.fori_loop(CUT_X, PAIRS, inner, 0)

    part = TOK // HN
    here = pl.ds(pl.multiple_of(hd * part, part), part)

    def scatter(own, got, k):
        return [
            send(own.at[q], got.at[d], y_s.at[k, d], y_r.at[k, d], (me, q))
            for q, d in zip(y_peers, range(HN - 1))
        ]

    def gather(own, got, out, k):
        out[here, :] = own[hd] + got[0] + got[1] + got[2]
        return [
            send(out.at[here], out.at[here], y_s.at[k, d], y_r.at[k, d], (me, q))
            for q, d in zip(y_peers, range(HN - 1))
        ]

    table = jnp.where(causal, et[...], 0.0)
    s_pair = split(s0_ref[...])
    dc = nn3(split(table.T), b_pair) + nn3((eh[...], el[...]), s_pair)
    for q in range(HN):
        own_c[q] = dc[q * part : (q + 1) * part]
    c_copies = scatter(own_c, got_c, 0)
    dbl[...] = nn3(split(table), c_pair)

    for copy in b_copies:
        copy.wait()
    for j in range(ZN):
        late = back[j]
        early = g1[j] + a1 * late
        rows = pl.ds(pl.multiple_of(core * HALF + j * SLICE, SLICE), SLICE)
        lat[rows, :] = jnp.where(even, early, late)
        other[j * SLICE : (j + 1) * SLICE, :] = jnp.where(even, late, early)
    c2 = send(other, lat.at[mine], pair_s.at[2], pair_r.at[2], mate)
    for copy in c_copies:
        copy.wait()
    c_copies = gather(own_c, got_c, dc_ref, 1)
    c2.wait()

    hi, lo = split(lat[...])
    lh[...] = hi
    ll[...] = lo
    db = nt3((txh[...], txl[...]), (hi, lo)) + dbl[...]
    for q in range(HN):
        own_b[q] = db[q * part : (q + 1) * part]
    d_copies = scatter(own_b, got_b, 2)

    top = iota((8, TILE), 0)

    def correct(p, carry):
        tile = tile_of(p)
        raw = nn3(b_pair, (lh[:, tile], ll[:, tile]))
        dx_ref[:, tile] = dx_ref[:, tile] + tail_ref[:, tile] * raw
        tx = txh[:, tile].astype(F32) + txl[:, tile].astype(F32)
        vh, vl = split(tx * raw)
        w[pl.ds(pl.multiple_of(p * 8, 8), 8), :] = v_ref[p] + nt(picker, vh) + nt(picker, vl)
        eg = (a_ref[:, tile] * lat[:, tile] + gt_ref[:, tile]).T
        eg_ref[tile, :] = eg
        product = eg * s0_ref[tile, :]
        one = jnp.sum(jnp.sum(product[:WIDTH], axis=0, keepdims=True), axis=1, keepdims=True)
        two = jnp.sum(jnp.sum(product[WIDTH:], axis=0, keepdims=True), axis=1, keepdims=True)
        first_g[pl.ds(pl.multiple_of(p * 8, 8), 8), :] = jnp.where(
            top == 0, one, jnp.where(top == 1, two, 0.0)
        )
        return carry

    lax.fori_loop(0, CUT_Y, correct, 0)
    for copy in d_copies:
        copy.wait()
    d_copies = gather(own_b, got_b, db_ref, 3)
    lax.fori_loop(CUT_Y, PAIRS, correct, 0)
    rates = prefix_sums(w[...], True) + first_g[:, 0:1]
    for h in range(HEADS):
        k = (h // 2) * 8 + h % 2
        dld_ref[h : h + 1, :] = rates[k : k + 1, :]
    for copy in c_copies:
        copy.wait()
    for copy in d_copies:
        copy.wait()


def run(x, ld, b, c, s0, dy):
    vm = pl.BlockSpec(memory_space=pltpu.VMEM)
    hbm = pl.BlockSpec(memory_space=pltpu.HBM)
    dma = pltpu.SemaphoreType.DMA
    shape = jax.ShapeDtypeStruct
    slab = pltpu.VMEM((ZN, SLICE, ROWS), F32)
    tall = pltpu.VMEM((TOK, ROWS), F32)
    tall16 = pltpu.VMEM((TOK, ROWS), BF16)
    state = pltpu.VMEM((STATE, ROWS), F32)
    quarter = TOK // HN
    return pl.pallas_call(
        main_kernel,
        out_shape=(
            OUT((TOK, ROWS), F32),
            OUT((HEADS, TOK), F32),
            OUT((TOK, STATE), F32),
            OUT((TOK, STATE), F32),
            OUT((ROWS, STATE), F32),
        ),
        in_specs=[hbm, vm, vm, vm, hbm, hbm],
        out_specs=(vm,) * 5,
        scratch_shapes=[
            tall,
            pltpu.VMEM((ROWS, STATE), F32),
            tall,
            state,
            pltpu.VMEM((1, ROWS), F32),
            tall16,
            tall16,
            tall,
            pltpu.VMEM((PAIRS, 8, TOK), F32),
            pltpu.VMEM((TOK, STATE), F32),
            pltpu.VMEM((32, TOK), F32),
            pltpu.VMEM((TOK, HEADS * TILE), F32),
            pltpu.VMEM((HEADS, 1, TOK), F32),
            pltpu.VMEM((TOK, TOK), F32),
            pltpu.VMEM((TOK, TOK), F32),
            tall16,
            tall16,
            pltpu.VMEM((1, TILE), F32),
            pltpu.VMEM((HALF, ROWS), F32),
            pltpu.VMEM((1, TILE), F32),
            slab,
            pltpu.VMEM((2, 1, TILE), F32),
            slab,
            slab,
            pltpu.VMEM((ZN, 2, 1, TILE), F32),
            slab,
            pltpu.VMEM((ZN, 1, ROWS), F32),
            pltpu.VMEM((XN, SLICE, ROWS), F32),
            pltpu.VMEM((XN, 1, ROWS), F32),
            slab,
            slab,
            pltpu.VMEM((HALF, ROWS), F32),
            state,
            pltpu.VMEM((STATE, ROWS), BF16),
            pltpu.VMEM((STATE, ROWS), BF16),
            pltpu.VMEM((PAIRS * 8, TOK), F32),
            pltpu.VMEM((PAIRS * 8, TILE), F32),
            pltpu.VMEM((HN, quarter, STATE), F32),
            pltpu.VMEM((HN - 1, quarter, STATE), F32),
            pltpu.VMEM((HN, quarter, STATE), F32),
            pltpu.VMEM((HN - 1, quarter, STATE), F32),
            dma((3,)),
            dma((3,)), dma((3,)),
            dma((2, ZN - 1)), dma((2, ZN - 1)),
            dma((2, XN - 1)), dma((2, XN - 1)),
            dma((ZN - 1,)), dma((ZN - 1,)),
            dma((4, HN - 1)), dma((4, HN - 1)),
        ],
        compiler_params=pltpu.CompilerParams(
            collective_id=0, has_side_effects=True, vmem_limit_bytes=VMEM_LIMIT
        ),
        name="main",
    )(x, ld, b, c, s0, dy)


def per_device(inputs, log_decay, b_proj, c_proj, entry_states, out_grad):
    s0 = entry_states.reshape(ROWS, STATE)
    dx, dld, db, dc, eg = run(inputs, log_decay, b_proj, c_proj, s0, out_grad)
    return (dx, dld, db, dc, eg.reshape(1, HEADS, WIDTH, STATE))


def solution(mesh):
    return jax.shard_map(
        per_device,
        mesh=mesh,
        in_specs=(
            P("seq", "head"),
            P("head", "seq"),
            P("seq", None),
            P("seq", None),
            P("seq", "head", None, None),
            P("seq", "head"),
        ),
        out_specs=(
            P("seq", "head"),
            P("head", "seq"),
            P("seq", None),
            P("seq", None),
            P("seq", "head", None, None),
        ),
        check_vma=False,
    )
```

```python
import functools

import jax
import jax.numpy as jnp
from jax import lax
from jax.experimental import pallas as pl
from jax.experimental.pallas import tpu as pltpu
from jax.sharding import PartitionSpec as P

F32 = jnp.float32
BF16 = jnp.bfloat16
MESH = pl.DeviceIdType.MESH
TOK = 512
HEADS = 20
WIDTH = 64
STATE = 128
ROWS = HEADS * WIDTH
PAIRS = HEADS // 2
TILE = 128
LOG2E = 1.4426950408889634
ZN = 8
XN = 4
HN = 4
HALF = STATE // 2
SLICE = HALF // ZN
LINE = 2 * ZN
PARTS = 2
PART_PAIRS = PAIRS // PARTS
PART = PART_PAIRS * TILE
CUTS = (4, 7, 7, 10)
VMEM_LIMIT = 58 * 1024 * 1024


def split(v):
    hi = v.astype(BF16)
    return hi, (v - hi.astype(F32)).astype(BF16)


def split3(v):
    hi = v.astype(BF16)
    rest = v - hi.astype(F32)
    mid = rest.astype(BF16)
    return hi, mid, (rest - mid.astype(F32)).astype(BF16)


def nn(a, b):
    return lax.dot_general(a, b, (((1,), (0,)), ((), ())), preferred_element_type=F32)


def nt(a, b):
    return lax.dot_general(a, b, (((1,), (1,)), ((), ())), preferred_element_type=F32)


def nn3(a, b):
    a_hi, a_lo = a
    b_hi, b_lo = b
    width = b_hi.shape[1]
    both = nn(a_hi, jnp.concatenate([b_hi, b_lo], axis=1))
    return both[:, :width] + both[:, width:] + nn(a_lo, b_hi)


def nt3(a, b):
    a_hi, a_lo = a
    b_hi, b_lo = b
    return nt(a_hi, b_hi) + nt(a_hi, b_lo) + nt(a_lo, b_hi)


def iota(shape, dim):
    return lax.broadcasted_iota(jnp.int32, shape, dim)


def prefix_sums(value, strict):
    rows = value.shape[0]
    a, b = iota((TILE, TILE), 0), iota((TILE, TILE), 1)
    upper = jnp.where(a < b if strict else a <= b, 1.0, 0.0).astype(BF16)
    tiles = []
    base = jnp.zeros((rows, 1), F32)
    for j in range(TOK // TILE):
        part = value[:, j * TILE : (j + 1) * TILE]
        hi, mid, lo = split3(part)
        inner = nn(hi, upper) + nn(mid, upper) + nn(lo, upper)
        tiles.append(inner + base)
        last = tiles[-1][:, TILE - 1 : TILE]
        base = last + part[:, TILE - 1 : TILE] if strict else last
    return jnp.concatenate(tiles, axis=1)


def pair_picker():
    row, lane = iota((8, TILE), 0), iota((8, TILE), 1)
    low = (row == 0) & (lane < WIDTH)
    high = (row == 1) & (lane >= WIDTH)
    return jnp.where(low | high, 1.0, 0.0).astype(BF16)


def main_kernel(
    x_hbm, ld_hbm, b_hbm, c_hbm, s0_hbm, dy_hbm,
    dx_ref, dld_ref, db_ref, dc_ref, eg_ref,
    x_ref, s0_ref, dy_ref, gt_ref, a_ref, txh, txl, tail_ref, v_ref, dbl,
    ld_ref, b_ref, c_ref, ld32, lanes, lx, lrow, cbt, et, eh, el,
    pg, chip, g1, zbuf, zl3, zrow, inside, fac, step, xg, xl, lbuf, back, other, lat,
    lh, ll, w, first_g, own_c, got_c, own_b, got_b,
    in_s, pair_s, pair_r, l_s, l_r, z_s, z_r, x_s, x_r, b_s, b_r, y_s, y_r,
):
    me, hd = lax.axis_index("seq"), lax.axis_index("head")
    core = lax.rem(me, 2)
    z = lax.rem(me // 2, ZN)
    x = me // (2 * ZN)
    even = core == 0

    def peer(px, pz, pc):
        return (px * 2 * ZN + pz * 2 + pc, hd)

    mate = peer(x, z, 1 - core)
    spot = z * 2 + core
    line = [lax.rem(spot + d, LINE) for d in range(1, LINE)]
    z_peers = [lax.rem(z + d, ZN) for d in range(1, ZN)]
    x_peers = [lax.rem(x + d, XN) for d in range(1, XN)]
    y_peers = [lax.rem(hd + d, HN) for d in range(1, HN)]
    barrier = pltpu.get_barrier_semaphore()
    everyone = (
        [peer(x, q // 2, lax.rem(q, 2)) for q in line]
        + [peer(q, z, core) for q in x_peers]
        + [(me, q) for q in y_peers]
    )

    def lanes_of(k):
        return slice(k * PART, (k + 1) * PART)

    smalls = [
        pltpu.make_async_copy(ld_hbm, ld_ref, in_s.at[PARTS + 2]),
        pltpu.make_async_copy(c_hbm, c_ref, in_s.at[PARTS + 3]),
        pltpu.make_async_copy(b_hbm, b_ref, in_s.at[PARTS + 4]),
    ]
    loads = [
        pltpu.make_async_copy(dy_hbm.at[:, lanes_of(k)], dy_ref.at[:, lanes_of(k)], in_s.at[k])
        for k in range(PARTS)
    ]
    smalls[0].start()
    smalls[1].start()
    for load in loads:
        load.start()
    smalls[2].start()
    for device in everyone:
        pl.semaphore_signal(barrier, inc=1, device_id=device, device_id_type=MESH)
    def send(src, dst, s, r, device):
        copy = pltpu.make_async_remote_copy(
            src_ref=src, dst_ref=dst, send_sem=s, recv_sem=r, device_id=device, device_id_type=MESH
        )
        copy.start()
        return copy

    first = iota((1, TILE), 1) < WIDTH
    smalls[0].wait()
    ld32[...] = jnp.zeros_like(ld32)
    ld32[0:HEADS, :] = ld_ref[...] * LOG2E
    cum = prefix_sums(ld32[...], False)
    for h in range(HEADS):
        lrow[h] = cum[h : h + 1, :]
    hi, mid, lo = split3(cum)
    stack = jnp.concatenate(
        [hi.astype(F32), mid.astype(F32), lo.astype(F32), jnp.zeros_like(cum)], axis=0
    )
    columns = stack.T
    zl3[spot] = columns[TOK - 1 : TOK, :]
    columns = columns.astype(BF16)
    pl.semaphore_wait(barrier, len(everyone))
    l_copies = [
        send(zl3.at[spot], zl3.at[spot], l_s.at[d], l_r.at[d], peer(x, q // 2, lax.rem(q, 2)))
        for q, d in zip(line, range(LINE - 1))
    ]
    narrow = (TILE, ROWS)
    spread = jnp.where((iota(narrow, 0) & 31) == (iota(narrow, 1) >> 6), 1.0, 0.0).astype(BF16)
    lanes[...] = spread
    smalls[1].wait()
    ct_pair = split(c_ref[...].T)

    def tile_of(p):
        return pl.ds(pl.multiple_of(p * TILE, TILE), TILE)

    def logs_of(p):
        return nn(columns, lanes[:, tile_of(p)])

    def starter(k):
        def start(p, carry):
            tile = tile_of(p + k * PART_PAIRS)
            e_pair = split(jnp.exp2(logs_of(p + k * PART_PAIRS)) * dy_ref[:, tile])
            eh[:, tile] = e_pair[0]
            el[:, tile] = e_pair[1]
            gt_ref[k, :, tile_of(p)] = nn3(ct_pair, e_pair)
            return carry

        return start

    away = pl.ds(pl.multiple_of((1 - core) * HALF, HALF), HALF)
    mine = pl.ds(pl.multiple_of(core * HALF, HALF), HALF)
    m_copies = []
    for k in range(PARTS):
        loads[k].wait()
        lax.fori_loop(0, PART_PAIRS, starter(k), 0)
        m_copies.append(send(gt_ref.at[k, away], pg.at[k], pair_s.at[0, k], pair_r.at[0, k], mate))
    rest = [
        pltpu.make_async_copy(x_hbm, x_ref, in_s.at[PARTS]),
        pltpu.make_async_copy(s0_hbm, s0_ref, in_s.at[PARTS + 1]),
    ]
    for load in rest:
        load.start()

    for copy in l_copies:
        copy.wait()
    line_logs = nn(jnp.concatenate([zl3[i] for i in range(LINE)], axis=0).astype(BF16), spread)
    log = jnp.zeros((1, ROWS), F32)
    for j in reversed(range(ZN)):
        one, two = line_logs[2 * j : 2 * j + 1], line_logs[2 * j + 1 : 2 * j + 2]
        zrow[2 * j] = one
        zrow[2 * j + 1] = two
        fac[j] = jnp.exp2(log)
        step[j] = jnp.exp2(one + two)
        log = log + (one + two)
    xl[x] = jnp.exp2(log)
    r_copies = [
        send(xl.at[x], xl.at[x], x_s.at[PARTS, d], x_r.at[PARTS, d], peer(q, z, core))
        for q, d in zip(x_peers, range(XN - 1))
    ]
    a0, a1 = jnp.exp2(zrow[2 * z]), jnp.exp2(zrow[2 * z + 1])
    a_ref[...] = jnp.where(even, a0, a1)

    z_copies = []
    for k in range(PARTS):
        m_copies[k].wait()
        for j in range(ZN):
            rows = pl.ds(pl.multiple_of(core * HALF + j * SLICE, SLICE), SLICE)
            part, mate_part = gt_ref[k, rows, :], pg[k, j * SLICE : (j + 1) * SLICE, :]
            later = jnp.where(even, mate_part, part)
            g1[k, j] = later
            chip[k, j] = jnp.where(even, part, mate_part) + a0[:, lanes_of(k)] * later
        z_copies.append(
            [
                send(chip.at[k, q], zbuf.at[k, z], z_s.at[k, d], z_r.at[k, d], peer(x, q, core))
                for q, d in zip(z_peers, range(ZN - 1))
            ]
        )
        zbuf[k, z] = chip[k, z]

    wide = (TILE, HEADS * TILE)
    spread = jnp.where((iota(wide, 0) & 31) == (iota(wide, 1) >> 7), 1.0, 0.0).astype(BF16)
    for k in range(HEADS // 4):
        part = slice(k * 4 * TILE, (k + 1) * 4 * TILE)
        lx[:, part] = nn(columns, spread[:, part])
    c_pair = split(c_ref[...])
    smalls[2].wait()
    b_pair = split(b_ref[...])
    causal = iota((TOK, TOK), 0) <= iota((TOK, TOK), 1)
    cbt[...] = jnp.where(causal, nt3(b_pair, c_pair), 0.0)
    et[...] = jnp.zeros_like(et)

    picker = jnp.concatenate([pair_picker()] * 2, axis=1)
    c_both = jnp.concatenate(c_pair, axis=1)
    b_both = jnp.concatenate(b_pair, axis=1)
    sub = iota((8, TOK), 0)

    def inner(p, carry):
        tile = tile_of(p)
        xv, dy = x_ref[:, tile], dy_ref[:, tile]
        both = logs_of(p)
        tail = jnp.exp2(both[TOK - 1 : TOK, :] - both)
        tail_ref[:, tile] = tail
        tx = split(tail * xv)
        txh[:, tile] = tx[0]
        txl[:, tile] = tx[1]
        xh, xlo = split(xv)
        dyh, dyl = split(dy)
        xh_f, dyh_f = xh.astype(F32), dyh.astype(F32)
        x_turn = pltpu.roll(xlo.astype(F32), WIDTH, 1)
        dy_turn = pltpu.roll(dyh_f, WIDTH, 1)
        dyl_f = dyl.astype(F32)
        zero = jnp.zeros_like(xv)
        dycat = jnp.concatenate([dyh, dyl], axis=1)
        left, right = [], []
        for k in range(2):
            here = first if k == 0 else jnp.logical_not(first)
            left.append(
                jnp.concatenate(
                    [jnp.where(here, xh_f, x_turn), jnp.where(here, xh_f, zero)], axis=1
                ).astype(BF16)
            )
            right.append(
                jnp.concatenate(
                    [jnp.where(here, dyh_f, dy_turn), jnp.where(here, dyl_f, zero)], axis=1
                ).astype(BF16)
            )
        zs = [[jnp.zeros((1, TILE), F32) for j in range(4)] for k in range(2)]
        blank = jnp.zeros((TILE, TILE), BF16)
        for i in range(2):
            r = i * 2 * TILE
            outs = []
            gained = [et[r + m * TILE : r + (m + 1) * TILE, r + m * TILE :] for m in range(2)]
            for k in range(2):
                grads = nt(left[k][r : r + 2 * TILE], right[k][r:])
                highs, lows = [], []
                for m in range(2):
                    q = r + m * TILE
                    grad = grads[m * TILE : (m + 1) * TILE, m * TILE :]
                    column = lx[q : q + TILE, tile_of(2 * p + k)]
                    row = lrow[2 * p + k][:, q:]
                    decay = []
                    for j in range((TOK - q) // TILE):
                        gap = row[:, j * TILE : (j + 1) * TILE] - column
                        decay.append(jnp.exp2(jnp.minimum(gap, 0.0) if j == 0 else gap))
                    decay = jnp.concatenate(decay, axis=1)
                    weight = decay * cbt[q : q + TILE, q:]
                    gained[m] = gained[m] + decay * grad
                    sums = jnp.sum(weight * grad, axis=0, keepdims=True)
                    for j in range((TOK - q) // TILE):
                        at = q // TILE + j
                        zs[k][at] = zs[k][at] + sums[:, j * TILE : (j + 1) * TILE]
                    wh, wl = split(weight)
                    highs.append(jnp.concatenate([blank, wh], axis=1) if m else wh)
                    lows.append(jnp.concatenate([blank, wl], axis=1) if m else wl)
                out = nn(jnp.concatenate(highs, axis=0), dycat[r:])
                low = nn(jnp.concatenate(lows, axis=0), dyh[r:])
                outs.append(out[:, :TILE] + out[:, TILE:] + low)
            for m in range(2):
                q = r + m * TILE
                et[q : q + TILE, q:] = gained[m]
            dx_ref[r : r + 2 * TILE, tile] = jnp.where(first, outs[0], outs[1])
        sh, sl = split(s0_ref[tile, :])
        both = nt(
            c_both,
            jnp.concatenate(
                [jnp.concatenate([sh, sh], axis=1), jnp.concatenate([sl, sl], axis=1)], axis=0
            ),
        )
        entering = both[:, :TILE] + both[:, TILE:]
        e = eh[:, tile].astype(F32) + el[:, tile].astype(F32)
        vh, vl = split(xv * dx_ref[:, tile] - e * entering)
        za, zb = jnp.concatenate(zs[0], axis=1), jnp.concatenate(zs[1], axis=1)
        v_ref[p] = (
            nt(picker, jnp.concatenate([vh, vl], axis=1))
            - jnp.where(sub == 0, za, jnp.where(sub == 1, zb, 0.0))
        )
        return carry

    for load in rest:
        load.wait()

    def line_scan(k):
        for copy in z_copies[k]:
            copy.wait()
        state = jnp.zeros((SLICE, PART), F32)
        for j in reversed(range(ZN)):
            inside[k, j] = state
            state = zbuf[k, j] + step[j][:, lanes_of(k)] * state
        xg[k, x] = state
        return [
            send(xg.at[k, x], xg.at[k, x], x_s.at[k, d], x_r.at[k, d], peer(q, z, core))
            for q, d in zip(x_peers, range(XN - 1))
        ]

    def line_back(k, copies):
        for copy in copies:
            copy.wait()
        entering = jnp.zeros((SLICE, PART), F32)
        for q in reversed(range(1, XN)):
            entering = jnp.where(q > x, xg[k, q] + xl[q][:, lanes_of(k)] * entering, entering)
        for j in range(ZN):
            lbuf[k, j] = inside[k, j] + fac[j][:, lanes_of(k)] * entering
        copies = [
            send(lbuf.at[k, q], back.at[k, z], b_s.at[k, d], b_r.at[k, d], peer(x, q, core))
            for q, d in zip(z_peers, range(ZN - 1))
        ]
        back[k, z] = lbuf[k, z]
        return copies

    lax.fori_loop(0, CUTS[0], inner, 0)
    x_copies = [line_scan(0)]
    lax.fori_loop(CUTS[0], CUTS[1], inner, 0)
    for copy in r_copies:
        copy.wait()
    b_copies = [line_back(0, x_copies[0])]
    lax.fori_loop(CUTS[1], CUTS[2], inner, 0)
    x_copies.append(line_scan(1))
    lax.fori_loop(CUTS[2], CUTS[3], inner, 0)
    b_copies.append(line_back(1, x_copies[1]))
    lax.fori_loop(CUTS[3], PAIRS, inner, 0)

    part = TOK // HN
    here = pl.ds(pl.multiple_of(hd * part, part), part)

    def scatter(own, got, k):
        return [
            send(own.at[q], got.at[d], y_s.at[k, d], y_r.at[k, d], (me, q))
            for q, d in zip(y_peers, range(HN - 1))
        ]

    def gather(own, got, out, k):
        out[here, :] = own[hd] + got[0] + got[1] + got[2]
        return [
            send(out.at[here], out.at[here], y_s.at[k, d], y_r.at[k, d], (me, q))
            for q, d in zip(y_peers, range(HN - 1))
        ]

    table = jnp.where(causal, et[...], 0.0)
    s_pair = split(s0_ref[...])
    dc = nn3(split(table.T), b_pair) + nn3((eh[...], el[...]), s_pair)
    for q in range(HN):
        own_c[q] = dc[q * part : (q + 1) * part]
    c_copies = scatter(own_c, got_c, 0)
    dbl[...] = nn3(split(table), c_pair)

    f_copies = []
    for k in range(PARTS):
        for copy in b_copies[k]:
            copy.wait()
        for j in range(ZN):
            late = back[k, j]
            early = g1[k, j] + a1[:, lanes_of(k)] * late
            rows = pl.ds(pl.multiple_of(core * HALF + j * SLICE, SLICE), SLICE)
            lat[k, rows, :] = jnp.where(even, early, late)
            other[k, j * SLICE : (j + 1) * SLICE, :] = jnp.where(even, late, early)
        f_copies.append(
            send(other.at[k], lat.at[k, mine], pair_s.at[1, k], pair_r.at[1, k], mate)
        )
    for copy in c_copies:
        copy.wait()
    c_copies = gather(own_c, got_c, dc_ref, 1)
    db = dbl[...]
    for k in range(PARTS):
        f_copies[k].wait()
        hi, lo = split(lat[k])
        lh[k] = hi
        ll[k] = lo
        both = nt(txh[:, lanes_of(k)], jnp.concatenate([hi, lo], axis=0))
        db = db + both[:, :STATE] + both[:, STATE:] + nt(txl[:, lanes_of(k)], hi)
    for q in range(HN):
        own_b[q] = db[q * part : (q + 1) * part]
    d_copies = scatter(own_b, got_b, 2)

    top = iota((8, TILE), 0)

    def corrector(k):
        def correct(p, carry):
            tile = tile_of(p + k * PART_PAIRS)
            spot = tile_of(p)
            late = jnp.concatenate([lh[k, :, spot], ll[k, :, spot]], axis=1)
            raw = nn(b_both, jnp.concatenate([late, late], axis=0))
            raw = raw[:, :TILE] + raw[:, TILE:]
            dx_ref[:, tile] = dx_ref[:, tile] + tail_ref[:, tile] * raw
            tx = txh[:, tile].astype(F32) + txl[:, tile].astype(F32)
            vh, vl = split(tx * raw)
            slot = pl.ds(pl.multiple_of((p + k * PART_PAIRS) * 8, 8), 8)
            w[slot, :] = v_ref[p + k * PART_PAIRS] + nt(
                picker, jnp.concatenate([vh, vl], axis=1)
            )
            eg = (a_ref[:, tile] * lat[k, :, spot] + gt_ref[k, :, spot]).T
            eg_ref[tile, :] = eg
            product = eg * s0_ref[tile, :]
            one = jnp.sum(jnp.sum(product[:WIDTH], axis=0, keepdims=True), axis=1, keepdims=True)
            two = jnp.sum(jnp.sum(product[WIDTH:], axis=0, keepdims=True), axis=1, keepdims=True)
            first_g[slot, :] = jnp.where(top == 0, one, jnp.where(top == 1, two, 0.0))
            return carry

        return correct

    lax.fori_loop(0, PART_PAIRS, corrector(0), 0)
    for copy in d_copies:
        copy.wait()
    d_copies = gather(own_b, got_b, db_ref, 3)
    lax.fori_loop(0, PART_PAIRS, corrector(1), 0)
    rates = prefix_sums(w[...], True) + first_g[:, 0:1]
    for h in range(HEADS):
        k = (h // 2) * 8 + h % 2
        dld_ref[h : h + 1, :] = rates[k : k + 1, :]
    for copy in c_copies:
        copy.wait()
    for copy in d_copies:
        copy.wait()


def run(x, ld, b, c, s0, dy):
    vm = pl.BlockSpec(memory_space=pltpu.VMEM)
    hbm = pl.BlockSpec(memory_space=pltpu.HBM)
    dma = pltpu.SemaphoreType.DMA
    shape = jax.ShapeDtypeStruct
    slab = pltpu.VMEM((PARTS, ZN, SLICE, PART), F32)
    half = pltpu.VMEM((PARTS, HALF, PART), F32)
    rows8 = pltpu.VMEM((ZN, 1, ROWS), F32)
    tall = pltpu.VMEM((TOK, ROWS), F32)
    tall16 = pltpu.VMEM((TOK, ROWS), BF16)
    state = pltpu.VMEM((PARTS, STATE, PART), F32)
    state16 = pltpu.VMEM((PARTS, STATE, PART), BF16)
    quarter = TOK // HN
    return pl.pallas_call(
        main_kernel,
        out_shape=(
            pltpu.VMEM((TOK, ROWS), F32),
            pltpu.VMEM((HEADS, TOK), F32),
            pltpu.VMEM((TOK, STATE), F32),
            pltpu.VMEM((TOK, STATE), F32),
            pltpu.VMEM((ROWS, STATE), F32),
        ),
        in_specs=[hbm] * 6,
        out_specs=(vm,) * 5,
        scratch_shapes=[
            tall,
            pltpu.VMEM((ROWS, STATE), F32),
            tall,
            state,
            pltpu.VMEM((1, ROWS), F32),
            tall16,
            tall16,
            tall,
            pltpu.VMEM((PAIRS, 8, TOK), F32),
            pltpu.VMEM((TOK, STATE), F32),
            pltpu.VMEM((HEADS, TOK), F32),
            pltpu.VMEM((TOK, STATE), F32),
            pltpu.VMEM((TOK, STATE), F32),
            pltpu.VMEM((32, TOK), F32),
            pltpu.VMEM((TILE, ROWS), BF16),
            pltpu.VMEM((TOK, HEADS * TILE), F32),
            pltpu.VMEM((HEADS, 1, TOK), F32),
            pltpu.VMEM((TOK, TOK), F32),
            pltpu.VMEM((TOK, TOK), F32),
            tall16,
            tall16,
            half,
            slab,
            slab,
            slab,
            pltpu.VMEM((LINE, 1, TILE), F32),
            pltpu.VMEM((LINE, 1, ROWS), F32),
            slab,
            rows8,
            rows8,
            pltpu.VMEM((PARTS, XN, SLICE, PART), F32),
            pltpu.VMEM((XN, 1, ROWS), F32),
            slab,
            slab,
            half,
            state,
            state16,
            state16,
            pltpu.VMEM((PAIRS * 8, TOK), F32),
            pltpu.VMEM((PAIRS * 8, TILE), F32),
            pltpu.VMEM((HN, quarter, STATE), F32),
            pltpu.VMEM((HN - 1, quarter, STATE), F32),
            pltpu.VMEM((HN, quarter, STATE), F32),
            pltpu.VMEM((HN - 1, quarter, STATE), F32),
            dma((PARTS + 5,)),
            dma((2, PARTS)), dma((2, PARTS)),
            dma((LINE - 1,)), dma((LINE - 1,)),
            dma((PARTS, ZN - 1)), dma((PARTS, ZN - 1)),
            dma((PARTS + 1, XN - 1)), dma((PARTS + 1, XN - 1)),
            dma((PARTS, ZN - 1)), dma((PARTS, ZN - 1)),
            dma((4, HN - 1)), dma((4, HN - 1)),
        ],
        compiler_params=pltpu.CompilerParams(
            collective_id=0, has_side_effects=True, vmem_limit_bytes=VMEM_LIMIT
        ),
        name="main",
    )(x, ld, b, c, s0, dy)


def out_kernel(*refs):
    sem = refs[-1]
    half = (len(refs) - 1) // 2
    copies = [
        pltpu.make_async_copy(refs[k], refs[half + k], sem.at[k]) for k in range(half)
    ]
    for copy in copies:
        copy.start()
    for copy in copies:
        copy.wait()


def store(*values):
    return pl.pallas_call(
        out_kernel,
        out_shape=tuple(jax.ShapeDtypeStruct(v.shape, v.dtype) for v in values),
        in_specs=[pl.BlockSpec(memory_space=pltpu.VMEM)] * len(values),
        out_specs=(pl.BlockSpec(memory_space=pltpu.HBM),) * len(values),
        scratch_shapes=[pltpu.SemaphoreType.DMA((len(values),))],
        compiler_params=pltpu.CompilerParams(vmem_limit_bytes=1024 * 1024),
        name="store",
    )(*values)


def per_device(inputs, log_decay, b_proj, c_proj, entry_states, out_grad):
    s0 = entry_states.reshape(ROWS, STATE)
    dx, dld, db, dc, eg = store(*run(inputs, log_decay, b_proj, c_proj, s0, out_grad))
    return (dx, dld, db, dc, eg.reshape(1, HEADS, WIDTH, STATE))


def solution(mesh):
    return jax.shard_map(
        per_device,
        mesh=mesh,
        in_specs=(
            P("seq", "head"),
            P("head", "seq"),
            P("seq", None),
            P("seq", None),
            P("seq", "head", None, None),
            P("seq", "head"),
        ),
        out_specs=(
            P("seq", "head"),
            P("head", "seq"),
            P("seq", None),
            P("seq", None),
            P("seq", "head", None, None),
        ),
        check_vma=False,
    )
```

```python
import functools

import jax
import jax.numpy as jnp
from jax import lax
from jax.experimental import pallas as pl
from jax.experimental.pallas import tpu as pltpu
from jax.sharding import PartitionSpec as P

F32 = jnp.float32
BF16 = jnp.bfloat16
MESH = pl.DeviceIdType.MESH
TOK = 512
HEADS = 20
WIDTH = 64
STATE = 128
ROWS = HEADS * WIDTH
PAIRS = HEADS // 2
TILE = 128
LOG2E = 1.4426950408889634
ZN = 8
XN = 4
HN = 4
HALF = STATE // 2
SLICE = HALF // ZN
LINE = 2 * ZN
PARTS = 2
PART_PAIRS = PAIRS // PARTS
PART = PART_PAIRS * TILE
CUTS = (4, 7, 7, 9)
VMEM_LIMIT = 58 * 1024 * 1024


def split(v):
    hi = v.astype(BF16)
    return hi, (v - hi.astype(F32)).astype(BF16)


def split3(v):
    hi = v.astype(BF16)
    rest = v - hi.astype(F32)
    mid = rest.astype(BF16)
    return hi, mid, (rest - mid.astype(F32)).astype(BF16)


def nn(a, b):
    return lax.dot_general(a, b, (((1,), (0,)), ((), ())), preferred_element_type=F32)


def nt(a, b):
    return lax.dot_general(a, b, (((1,), (1,)), ((), ())), preferred_element_type=F32)


def nn3(a, b):
    a_hi, a_lo = a
    b_hi, b_lo = b
    width = b_hi.shape[1]
    both = nn(a_hi, jnp.concatenate([b_hi, b_lo], axis=1))
    return both[:, :width] + both[:, width:] + nn(a_lo, b_hi)


def nt3(a, b):
    a_hi, a_lo = a
    b_hi, b_lo = b
    return nt(a_hi, b_hi) + nt(a_hi, b_lo) + nt(a_lo, b_hi)


def iota(shape, dim):
    return lax.broadcasted_iota(jnp.int32, shape, dim)


def prefix_sums(value, strict):
    rows = value.shape[0]
    a, b = iota((TILE, TILE), 0), iota((TILE, TILE), 1)
    upper = jnp.where(a < b if strict else a <= b, 1.0, 0.0).astype(BF16)
    tiles = []
    base = jnp.zeros((rows, 1), F32)
    for j in range(TOK // TILE):
        part = value[:, j * TILE : (j + 1) * TILE]
        hi, mid, lo = split3(part)
        inner = nn(hi, upper) + nn(mid, upper) + nn(lo, upper)
        tiles.append(inner + base)
        last = tiles[-1][:, TILE - 1 : TILE]
        base = last + part[:, TILE - 1 : TILE] if strict else last
    return jnp.concatenate(tiles, axis=1)


def pair_picker():
    row, lane = iota((8, TILE), 0), iota((8, TILE), 1)
    low = (row == 0) & (lane < WIDTH)
    high = (row == 1) & (lane >= WIDTH)
    return jnp.where(low | high, 1.0, 0.0).astype(BF16)


def main_kernel(
    x_hbm, ld_hbm, b_hbm, c_hbm, s0_hbm, dy_hbm,
    dx_ref, dld_ref, db_ref, dc_ref, eg_ref,
    x_ref, s0_ref, dy_ref, gt_ref, a_ref, txh, txl, tail_ref, v_ref, dbl,
    ld_ref, b_ref, c_ref, ld32, lanes, lx, lrow, cbt, et, eh, el,
    pg, chip, g1, zbuf, zl3, zrow, inside, fac, step, xg, xl, lbuf, back, other, lat,
    lh, ll, w, first_g, own_c, got_c, own_b, got_b,
    in_s, pair_s, pair_r, l_s, l_r, z_s, z_r, x_s, x_r, b_s, b_r, y_s, y_r,
):
    me, hd = lax.axis_index("seq"), lax.axis_index("head")
    core = lax.rem(me, 2)
    z = lax.rem(me // 2, ZN)
    x = me // (2 * ZN)
    even = core == 0

    def peer(px, pz, pc):
        return (px * 2 * ZN + pz * 2 + pc, hd)

    mate = peer(x, z, 1 - core)
    spot = z * 2 + core
    line = [lax.rem(spot + d, LINE) for d in range(1, LINE)]
    z_peers = [lax.rem(z + d, ZN) for d in (4, 3, 5, 2, 6, 1, 7)]
    x_peers = [lax.rem(x + d, XN) for d in (2, 1, 3)]
    y_peers = [lax.rem(hd + d, HN) for d in (2, 1, 3)]
    barrier = pltpu.get_barrier_semaphore()
    everyone = (
        [peer(x, q // 2, lax.rem(q, 2)) for q in line]
        + [peer(q, z, core) for q in x_peers]
        + [(me, q) for q in y_peers]
    )

    def lanes_of(k):
        return slice(k * PART, (k + 1) * PART)

    smalls = [
        pltpu.make_async_copy(ld_hbm, ld_ref, in_s.at[PARTS + 2]),
        pltpu.make_async_copy(c_hbm, c_ref, in_s.at[PARTS + 3]),
        pltpu.make_async_copy(b_hbm, b_ref, in_s.at[PARTS + 4]),
    ]
    loads = [
        pltpu.make_async_copy(dy_hbm.at[:, lanes_of(k)], dy_ref.at[:, lanes_of(k)], in_s.at[k])
        for k in range(PARTS)
    ]
    smalls[0].start()
    smalls[1].start()
    for load in loads:
        load.start()
    smalls[2].start()
    for device in everyone:
        pl.semaphore_signal(barrier, inc=1, device_id=device, device_id_type=MESH)

    def send(src, dst, s, r, device):
        copy = pltpu.make_async_remote_copy(
            src_ref=src, dst_ref=dst, send_sem=s, recv_sem=r, device_id=device, device_id_type=MESH
        )
        copy.start()
        return copy

    first = iota((1, TILE), 1) < WIDTH
    smalls[0].wait()
    ld32[...] = jnp.zeros_like(ld32)
    ld32[0:HEADS, :] = ld_ref[...] * LOG2E
    cum = prefix_sums(ld32[...], False)
    for h in range(HEADS):
        lrow[h] = cum[h : h + 1, :]
    hi, mid, lo = split3(cum)
    stack = jnp.concatenate(
        [hi.astype(F32), mid.astype(F32), lo.astype(F32), jnp.zeros_like(cum)], axis=0
    )
    columns = stack.T
    zl3[spot] = columns[TOK - 1 : TOK, :]
    columns = columns.astype(BF16)
    narrow = (TILE, ROWS)
    spread = jnp.where((iota(narrow, 0) & 31) == (iota(narrow, 1) >> 6), 1.0, 0.0).astype(BF16)
    lanes[...] = spread
    smalls[1].wait()
    ct_pair = split(c_ref[...].T)

    def tile_of(p):
        return pl.ds(pl.multiple_of(p * TILE, TILE), TILE)

    def logs_of(p):
        return nn(columns, lanes[:, tile_of(p)])

    def starter(k):
        def start(p, carry):
            tile = tile_of(p + k * PART_PAIRS)
            e_pair = split(jnp.exp2(logs_of(p + k * PART_PAIRS)) * dy_ref[:, tile])
            eh[:, tile] = e_pair[0]
            el[:, tile] = e_pair[1]
            gt_ref[k, :, tile_of(p)] = nn3(ct_pair, e_pair)
            return carry

        return start

    away = pl.ds(pl.multiple_of((1 - core) * HALF, HALF), HALF)
    mine = pl.ds(pl.multiple_of(core * HALF, HALF), HALF)
    m_copies = []
    for k in range(PARTS):
        loads[k].wait()
        lax.fori_loop(0, PART_PAIRS, starter(k), 0)
        if k == 0:
            pl.semaphore_wait(barrier, len(everyone))
            l_copies = [
                send(zl3.at[spot], zl3.at[spot], l_s.at[d], l_r.at[d], peer(x, q // 2, lax.rem(q, 2)))
                for q, d in zip(line, range(LINE - 1))
            ]
        m_copies.append(send(gt_ref.at[k, away], pg.at[k], pair_s.at[0, k], pair_r.at[0, k], mate))
    rest = [
        pltpu.make_async_copy(x_hbm, x_ref, in_s.at[PARTS]),
        pltpu.make_async_copy(s0_hbm, s0_ref, in_s.at[PARTS + 1]),
    ]
    for load in rest:
        load.start()

    for copy in l_copies:
        copy.wait()
    line_logs = nn(jnp.concatenate([zl3[i] for i in range(LINE)], axis=0).astype(BF16), spread)
    log = jnp.zeros((1, ROWS), F32)
    for j in reversed(range(ZN)):
        one, two = line_logs[2 * j : 2 * j + 1], line_logs[2 * j + 1 : 2 * j + 2]
        zrow[2 * j] = one
        zrow[2 * j + 1] = two
        fac[j] = jnp.exp2(log)
        step[j] = jnp.exp2(one + two)
        log = log + (one + two)
    xl[x] = jnp.exp2(log)
    r_copies = [
        send(xl.at[x], xl.at[x], x_s.at[PARTS, d], x_r.at[PARTS, d], peer(q, z, core))
        for q, d in zip(x_peers, range(XN - 1))
    ]
    a0, a1 = jnp.exp2(zrow[2 * z]), jnp.exp2(zrow[2 * z + 1])
    a_ref[...] = jnp.where(even, a0, a1)

    z_copies = []
    for k in range(PARTS):
        m_copies[k].wait()
        for j in range(ZN):
            rows = pl.ds(pl.multiple_of(core * HALF + j * SLICE, SLICE), SLICE)
            part, mate_part = gt_ref[k, rows, :], pg[k, j * SLICE : (j + 1) * SLICE, :]
            later = jnp.where(even, mate_part, part)
            g1[k, j] = later
            chip[k, j] = jnp.where(even, part, mate_part) + a0[:, lanes_of(k)] * later
        z_copies.append(
            [
                send(chip.at[k, q], zbuf.at[k, z], z_s.at[k, d], z_r.at[k, d], peer(x, q, core))
                for q, d in zip(z_peers, range(ZN - 1))
            ]
        )
        zbuf[k, z] = chip[k, z]

    wide = (TILE, HEADS * TILE)
    spread = jnp.where((iota(wide, 0) & 31) == (iota(wide, 1) >> 7), 1.0, 0.0).astype(BF16)
    for k in range(HEADS // 4):
        part = slice(k * 4 * TILE, (k + 1) * 4 * TILE)
        lx[:, part] = nn(columns, spread[:, part])
    c_pair = split(c_ref[...])
    smalls[2].wait()
    b_pair = split(b_ref[...])
    causal = iota((TOK, TOK), 0) <= iota((TOK, TOK), 1)
    cbt[...] = jnp.where(causal, nt3(b_pair, c_pair), 0.0)
    et[...] = jnp.zeros_like(et)

    picker = jnp.concatenate([pair_picker()] * 2, axis=1)
    c_both = jnp.concatenate(c_pair, axis=1)
    b_both = jnp.concatenate(b_pair, axis=1)
    sub = iota((8, TOK), 0)

    def inner(p, carry):
        tile = tile_of(p)
        xv, dy = x_ref[:, tile], dy_ref[:, tile]
        both = logs_of(p)
        tail = jnp.exp2(both[TOK - 1 : TOK, :] - both)
        tail_ref[:, tile] = tail
        tx = split(tail * xv)
        txh[:, tile] = tx[0]
        txl[:, tile] = tx[1]
        xh, xlo = split(xv)
        dyh, dyl = split(dy)
        xh_f, dyh_f = xh.astype(F32), dyh.astype(F32)
        x_turn = pltpu.roll(xlo.astype(F32), WIDTH, 1)
        dy_turn = pltpu.roll(dyh_f, WIDTH, 1)
        dyl_f = dyl.astype(F32)
        zero = jnp.zeros_like(xv)
        dycat = jnp.concatenate([dyh, dyl], axis=1)
        left, right = [], []
        for k in range(2):
            here = first if k == 0 else jnp.logical_not(first)
            left.append(
                jnp.concatenate(
                    [jnp.where(here, xh_f, x_turn), jnp.where(here, xh_f, zero)], axis=1
                ).astype(BF16)
            )
            right.append(
                jnp.concatenate(
                    [jnp.where(here, dyh_f, dy_turn), jnp.where(here, dyl_f, zero)], axis=1
                ).astype(BF16)
            )
        zs = [[jnp.zeros((1, TILE), F32) for j in range(4)] for k in range(2)]
        blank = jnp.zeros((TILE, TILE), BF16)
        for i in range(2):
            r = i * 2 * TILE
            outs = []
            gained = [et[r + m * TILE : r + (m + 1) * TILE, r + m * TILE :] for m in range(2)]
            for k in range(2):
                grads = nt(left[k][r : r + 2 * TILE], right[k][r:])
                highs, lows = [], []
                for m in range(2):
                    q = r + m * TILE
                    grad = grads[m * TILE : (m + 1) * TILE, m * TILE :]
                    column = lx[q : q + TILE, tile_of(2 * p + k)]
                    row = lrow[2 * p + k][:, q:]
                    decay = []
                    for j in range((TOK - q) // TILE):
                        gap = row[:, j * TILE : (j + 1) * TILE] - column
                        decay.append(jnp.exp2(jnp.minimum(gap, 0.0) if j == 0 else gap))
                    decay = jnp.concatenate(decay, axis=1)
                    weight = decay * cbt[q : q + TILE, q:]
                    gained[m] = gained[m] + decay * grad
                    sums = jnp.sum(weight * grad, axis=0, keepdims=True)
                    for j in range((TOK - q) // TILE):
                        at = q // TILE + j
                        zs[k][at] = zs[k][at] + sums[:, j * TILE : (j + 1) * TILE]
                    wh, wl = split(weight)
                    highs.append(jnp.concatenate([blank, wh], axis=1) if m else wh)
                    lows.append(jnp.concatenate([blank, wl], axis=1) if m else wl)
                out = nn(jnp.concatenate(highs, axis=0), dycat[r:])
                low = nn(jnp.concatenate(lows, axis=0), dyh[r:])
                outs.append(out[:, :TILE] + out[:, TILE:] + low)
            for m in range(2):
                q = r + m * TILE
                et[q : q + TILE, q:] = gained[m]
            dx_ref[r : r + 2 * TILE, tile] = jnp.where(first, outs[0], outs[1])
        sh, sl = split(s0_ref[tile, :])
        both = nt(
            c_both,
            jnp.concatenate(
                [jnp.concatenate([sh, sh], axis=1), jnp.concatenate([sl, sl], axis=1)], axis=0
            ),
        )
        entering = both[:, :TILE] + both[:, TILE:]
        e = eh[:, tile].astype(F32) + el[:, tile].astype(F32)
        vh, vl = split(xv * dx_ref[:, tile] - e * entering)
        za, zb = jnp.concatenate(zs[0], axis=1), jnp.concatenate(zs[1], axis=1)
        v_ref[p] = (
            nt(picker, jnp.concatenate([vh, vl], axis=1))
            - jnp.where(sub == 0, za, jnp.where(sub == 1, zb, 0.0))
        )
        return carry

    for load in rest:
        load.wait()

    def line_scan(k):
        for copy in z_copies[k]:
            copy.wait()
        state = jnp.zeros((SLICE, PART), F32)
        for j in reversed(range(ZN)):
            inside[k, j] = state
            state = zbuf[k, j] + step[j][:, lanes_of(k)] * state
        xg[k, x] = state
        return [
            send(xg.at[k, x], xg.at[k, x], x_s.at[k, d], x_r.at[k, d], peer(q, z, core))
            for q, d in zip(x_peers, range(XN - 1))
        ]

    def line_back(k, copies):
        for copy in copies:
            copy.wait()
        entering = jnp.zeros((SLICE, PART), F32)
        for q in reversed(range(1, XN)):
            entering = jnp.where(q > x, xg[k, q] + xl[q][:, lanes_of(k)] * entering, entering)
        for j in range(ZN):
            lbuf[k, j] = inside[k, j] + fac[j][:, lanes_of(k)] * entering
        copies = [
            send(lbuf.at[k, q], back.at[k, z], b_s.at[k, d], b_r.at[k, d], peer(x, q, core))
            for q, d in zip(z_peers, range(ZN - 1))
        ]
        back[k, z] = lbuf[k, z]
        return copies

    lax.fori_loop(0, CUTS[0], inner, 0)
    x_copies = [line_scan(0)]
    lax.fori_loop(CUTS[0], CUTS[1], inner, 0)
    for copy in r_copies:
        copy.wait()
    b_copies = [line_back(0, x_copies[0])]
    lax.fori_loop(CUTS[1], CUTS[2], inner, 0)
    x_copies.append(line_scan(1))
    lax.fori_loop(CUTS[2], CUTS[3], inner, 0)
    b_copies.append(line_back(1, x_copies[1]))
    lax.fori_loop(CUTS[3], PAIRS, inner, 0)

    part = TOK // HN
    here = pl.ds(pl.multiple_of(hd * part, part), part)

    def scatter(own, got, k):
        return [
            send(own.at[q], got.at[d], y_s.at[k, d], y_r.at[k, d], (me, q))
            for q, d in zip(y_peers, range(HN - 1))
        ]

    def gather(own, got, out, k):
        out[here, :] = own[hd] + got[0] + got[1] + got[2]
        return [
            send(out.at[here], out.at[here], y_s.at[k, d], y_r.at[k, d], (me, q))
            for q, d in zip(y_peers, range(HN - 1))
        ]

    table = jnp.where(causal, et[...], 0.0)
    s_pair = split(s0_ref[...])
    dc = nn3(split(table.T), b_pair) + nn3((eh[...], el[...]), s_pair)
    for q in range(HN):
        own_c[q] = dc[q * part : (q + 1) * part]
    c_copies = scatter(own_c, got_c, 0)
    dbl[...] = nn3(split(table), c_pair)

    f_copies = []
    for k in range(PARTS):
        for copy in b_copies[k]:
            copy.wait()
        for j in range(ZN):
            late = back[k, j]
            early = g1[k, j] + a1[:, lanes_of(k)] * late
            rows = pl.ds(pl.multiple_of(core * HALF + j * SLICE, SLICE), SLICE)
            lat[k, rows, :] = jnp.where(even, early, late)
            other[k, j * SLICE : (j + 1) * SLICE, :] = jnp.where(even, late, early)
        f_copies.append(
            send(other.at[k], lat.at[k, mine], pair_s.at[1, k], pair_r.at[1, k], mate)
        )
    for copy in c_copies:
        copy.wait()
    c_copies = gather(own_c, got_c, dc_ref, 1)
    db = dbl[...]
    for k in range(PARTS):
        f_copies[k].wait()
        hi, lo = split(lat[k])
        lh[k] = hi
        ll[k] = lo
        both = nt(txh[:, lanes_of(k)], jnp.concatenate([hi, lo], axis=0))
        db = db + both[:, :STATE] + both[:, STATE:] + nt(txl[:, lanes_of(k)], hi)
    for q in range(HN):
        own_b[q] = db[q * part : (q + 1) * part]
    d_copies = scatter(own_b, got_b, 2)

    top = iota((8, TILE), 0)

    def corrector(k):
        def correct(p, carry):
            tile = tile_of(p + k * PART_PAIRS)
            spot = tile_of(p)
            late = jnp.concatenate([lh[k, :, spot], ll[k, :, spot]], axis=1)
            raw = nn(b_both, jnp.concatenate([late, late], axis=0))
            raw = raw[:, :TILE] + raw[:, TILE:]
            dx_ref[:, tile] = dx_ref[:, tile] + tail_ref[:, tile] * raw
            tx = txh[:, tile].astype(F32) + txl[:, tile].astype(F32)
            vh, vl = split(tx * raw)
            slot = pl.ds(pl.multiple_of((p + k * PART_PAIRS) * 8, 8), 8)
            w[slot, :] = v_ref[p + k * PART_PAIRS] + nt(
                picker, jnp.concatenate([vh, vl], axis=1)
            )
            eg = (a_ref[:, tile] * lat[k, :, spot] + gt_ref[k, :, spot]).T
            eg_ref[tile, :] = eg
            product = eg * s0_ref[tile, :]
            one = jnp.sum(jnp.sum(product[:WIDTH], axis=0, keepdims=True), axis=1, keepdims=True)
            two = jnp.sum(jnp.sum(product[WIDTH:], axis=0, keepdims=True), axis=1, keepdims=True)
            first_g[slot, :] = jnp.where(top == 0, one, jnp.where(top == 1, two, 0.0))
            return carry

        return correct

    lax.fori_loop(0, PART_PAIRS, corrector(0), 0)
    for copy in d_copies:
        copy.wait()
    d_copies = gather(own_b, got_b, db_ref, 3)
    lax.fori_loop(0, PART_PAIRS, corrector(1), 0)
    rates = prefix_sums(w[...], True) + first_g[:, 0:1]
    for h in range(HEADS):
        k = (h // 2) * 8 + h % 2
        dld_ref[h : h + 1, :] = rates[k : k + 1, :]
    for copy in c_copies:
        copy.wait()
    for copy in d_copies:
        copy.wait()


def run(x, ld, b, c, s0, dy):
    vm = pl.BlockSpec(memory_space=pltpu.VMEM)
    hbm = pl.BlockSpec(memory_space=pltpu.HBM)
    dma = pltpu.SemaphoreType.DMA
    shape = jax.ShapeDtypeStruct
    slab = pltpu.VMEM((PARTS, ZN, SLICE, PART), F32)
    half = pltpu.VMEM((PARTS, HALF, PART), F32)
    rows8 = pltpu.VMEM((ZN, 1, ROWS), F32)
    tall = pltpu.VMEM((TOK, ROWS), F32)
    tall16 = pltpu.VMEM((TOK, ROWS), BF16)
    state = pltpu.VMEM((PARTS, STATE, PART), F32)
    state16 = pltpu.VMEM((PARTS, STATE, PART), BF16)
    quarter = TOK // HN
    return pl.pallas_call(
        main_kernel,
        out_shape=(
            pltpu.VMEM((TOK, ROWS), F32),
            pltpu.VMEM((HEADS, TOK), F32),
            pltpu.VMEM((TOK, STATE), F32),
            pltpu.VMEM((TOK, STATE), F32),
            pltpu.VMEM((ROWS, STATE), F32),
        ),
        in_specs=[hbm] * 6,
        out_specs=(vm,) * 5,
        scratch_shapes=[
            tall,
            pltpu.VMEM((ROWS, STATE), F32),
            tall,
            state,
            pltpu.VMEM((1, ROWS), F32),
            tall16,
            tall16,
            tall,
            pltpu.VMEM((PAIRS, 8, TOK), F32),
            pltpu.VMEM((TOK, STATE), F32),
            pltpu.VMEM((HEADS, TOK), F32),
            pltpu.VMEM((TOK, STATE), F32),
            pltpu.VMEM((TOK, STATE), F32),
            pltpu.VMEM((32, TOK), F32),
            pltpu.VMEM((TILE, ROWS), BF16),
            pltpu.VMEM((TOK, HEADS * TILE), F32),
            pltpu.VMEM((HEADS, 1, TOK), F32),
            pltpu.VMEM((TOK, TOK), F32),
            pltpu.VMEM((TOK, TOK), F32),
            tall16,
            tall16,
            half,
            slab,
            slab,
            slab,
            pltpu.VMEM((LINE, 1, TILE), F32),
            pltpu.VMEM((LINE, 1, ROWS), F32),
            slab,
            rows8,
            rows8,
            pltpu.VMEM((PARTS, XN, SLICE, PART), F32),
            pltpu.VMEM((XN, 1, ROWS), F32),
            slab,
            slab,
            half,
            state,
            state16,
            state16,
            pltpu.VMEM((PAIRS * 8, TOK), F32),
            pltpu.VMEM((PAIRS * 8, TILE), F32),
            pltpu.VMEM((HN, quarter, STATE), F32),
            pltpu.VMEM((HN - 1, quarter, STATE), F32),
            pltpu.VMEM((HN, quarter, STATE), F32),
            pltpu.VMEM((HN - 1, quarter, STATE), F32),
            dma((PARTS + 5,)),
            dma((2, PARTS)), dma((2, PARTS)),
            dma((LINE - 1,)), dma((LINE - 1,)),
            dma((PARTS, ZN - 1)), dma((PARTS, ZN - 1)),
            dma((PARTS + 1, XN - 1)), dma((PARTS + 1, XN - 1)),
            dma((PARTS, ZN - 1)), dma((PARTS, ZN - 1)),
            dma((4, HN - 1)), dma((4, HN - 1)),
        ],
        compiler_params=pltpu.CompilerParams(
            collective_id=0, has_side_effects=True, vmem_limit_bytes=VMEM_LIMIT
        ),
        name="main",
    )(x, ld, b, c, s0, dy)


def out_kernel(*refs):
    sem = refs[-1]
    half = (len(refs) - 1) // 2
    copies = [
        pltpu.make_async_copy(refs[k], refs[half + k], sem.at[k]) for k in range(half)
    ]
    for copy in copies:
        copy.start()
    for copy in copies:
        copy.wait()


def store(*values):
    return pl.pallas_call(
        out_kernel,
        out_shape=tuple(jax.ShapeDtypeStruct(v.shape, v.dtype) for v in values),
        in_specs=[pl.BlockSpec(memory_space=pltpu.VMEM)] * len(values),
        out_specs=(pl.BlockSpec(memory_space=pltpu.HBM),) * len(values),
        scratch_shapes=[pltpu.SemaphoreType.DMA((len(values),))],
        compiler_params=pltpu.CompilerParams(vmem_limit_bytes=1024 * 1024),
        name="store",
    )(*values)


def per_device(inputs, log_decay, b_proj, c_proj, entry_states, out_grad):
    s0 = entry_states.reshape(ROWS, STATE)
    dx, dld, db, dc, eg = store(*run(inputs, log_decay, b_proj, c_proj, s0, out_grad))
    return (dx, dld, db, dc, eg.reshape(1, HEADS, WIDTH, STATE))


def solution(mesh):
    return jax.shard_map(
        per_device,
        mesh=mesh,
        in_specs=(
            P("seq", "head"),
            P("head", "seq"),
            P("seq", None),
            P("seq", None),
            P("seq", "head", None, None),
            P("seq", "head"),
        ),
        out_specs=(
            P("seq", "head"),
            P("head", "seq"),
            P("seq", None),
            P("seq", None),
            P("seq", "head", None, None),
        ),
        check_vma=False,
    )
```

```python
import functools

import jax
import jax.numpy as jnp
from jax import lax
from jax.experimental import pallas as pl
from jax.experimental.pallas import tpu as pltpu
from jax.sharding import PartitionSpec as P

F32 = jnp.float32
BF16 = jnp.bfloat16
MESH = pl.DeviceIdType.MESH
TOK = 512
HEADS = 20
WIDTH = 64
STATE = 128
ROWS = HEADS * WIDTH
PAIRS = HEADS // 2
TILE = 128
LOG2E = 1.4426950408889634
ZN = 8
XN = 4
HN = 4
HALF = STATE // 2
SLICE = HALF // ZN
LINE = 2 * ZN
PARTS = 2
PART_PAIRS = PAIRS // PARTS
PART = PART_PAIRS * TILE
CUTS = (4, 7, 7, 8)
VMEM_LIMIT = 58 * 1024 * 1024


def split(v):
    hi = v.astype(BF16)
    return hi, (v - hi.astype(F32)).astype(BF16)


def split3(v):
    hi = v.astype(BF16)
    rest = v - hi.astype(F32)
    mid = rest.astype(BF16)
    return hi, mid, (rest - mid.astype(F32)).astype(BF16)


def nn(a, b):
    return lax.dot_general(a, b, (((1,), (0,)), ((), ())), preferred_element_type=F32)


def nt(a, b):
    return lax.dot_general(a, b, (((1,), (1,)), ((), ())), preferred_element_type=F32)


def nn3(a, b):
    a_hi, a_lo = a
    b_hi, b_lo = b
    width = b_hi.shape[1]
    both = nn(a_hi, jnp.concatenate([b_hi, b_lo], axis=1))
    return both[:, :width] + both[:, width:] + nn(a_lo, b_hi)


def nt3(a, b):
    a_hi, a_lo = a
    b_hi, b_lo = b
    return nt(a_hi, b_hi) + nt(a_hi, b_lo) + nt(a_lo, b_hi)


def iota(shape, dim):
    return lax.broadcasted_iota(jnp.int32, shape, dim)


def prefix_sums(value, strict):
    rows = value.shape[0]
    a, b = iota((TILE, TILE), 0), iota((TILE, TILE), 1)
    upper = jnp.where(a < b if strict else a <= b, 1.0, 0.0).astype(BF16)
    tiles = []
    base = jnp.zeros((rows, 1), F32)
    for j in range(TOK // TILE):
        part = value[:, j * TILE : (j + 1) * TILE]
        hi, mid, lo = split3(part)
        inner = nn(hi, upper) + nn(mid, upper) + nn(lo, upper)
        tiles.append(inner + base)
        last = tiles[-1][:, TILE - 1 : TILE]
        base = last + part[:, TILE - 1 : TILE] if strict else last
    return jnp.concatenate(tiles, axis=1)


def pair_picker():
    row, lane = iota((8, TILE), 0), iota((8, TILE), 1)
    low = (row == 0) & (lane < WIDTH)
    high = (row == 1) & (lane >= WIDTH)
    return jnp.where(low | high, 1.0, 0.0).astype(BF16)


def main_kernel(
    x_hbm, ld_hbm, b_hbm, c_hbm, s0_hbm, dy_hbm,
    dx_ref, dld_ref, db_ref, dc_ref, eg_ref,
    x_ref, s0_ref, dy_ref, gt_ref, a_ref, txh, txl, tail_ref, v_ref, dbl,
    ld_ref, b_ref, c_ref, ld32, lanes, lx, lrow, cbt, et, eh, el,
    pg, chip, g1, zbuf, zl3, zrow, inside, fac, step, xg, xl, lbuf, back, other, lat,
    lh, ll, w, first_g, own_c, got_c, own_b, got_b,
    in_s, pair_s, pair_r, l_s, l_r, z_s, z_r, x_s, x_r, b_s, b_r, y_s, y_r,
):
    me, hd = lax.axis_index("seq"), lax.axis_index("head")
    core = lax.rem(me, 2)
    z = lax.rem(me // 2, ZN)
    x = me // (2 * ZN)
    even = core == 0

    def peer(px, pz, pc):
        return (px * 2 * ZN + pz * 2 + pc, hd)

    mate = peer(x, z, 1 - core)
    spot = z * 2 + core
    line = [lax.rem(spot + d, LINE) for d in range(1, LINE)]
    z_peers = [lax.rem(z + d, ZN) for d in (4, 3, 5, 2, 6, 1, 7)]
    x_peers = [lax.rem(x + d, XN) for d in (2, 1, 3)]
    y_peers = [lax.rem(hd + d, HN) for d in (2, 1, 3)]
    barrier = pltpu.get_barrier_semaphore()
    everyone = (
        [peer(x, q // 2, lax.rem(q, 2)) for q in line]
        + [peer(q, z, core) for q in x_peers]
        + [(me, q) for q in y_peers]
    )

    def lanes_of(k):
        return slice(k * PART, (k + 1) * PART)

    smalls = [
        pltpu.make_async_copy(ld_hbm, ld_ref, in_s.at[PARTS + 2]),
        pltpu.make_async_copy(c_hbm, c_ref, in_s.at[PARTS + 3]),
        pltpu.make_async_copy(b_hbm, b_ref, in_s.at[PARTS + 4]),
    ]
    loads = [
        pltpu.make_async_copy(dy_hbm.at[:, lanes_of(k)], dy_ref.at[:, lanes_of(k)], in_s.at[k])
        for k in range(PARTS)
    ]
    smalls[0].start()
    smalls[1].start()
    for load in loads:
        load.start()
    smalls[2].start()
    for device in everyone:
        pl.semaphore_signal(barrier, inc=1, device_id=device, device_id_type=MESH)

    def send(src, dst, s, r, device):
        copy = pltpu.make_async_remote_copy(
            src_ref=src, dst_ref=dst, send_sem=s, recv_sem=r, device_id=device, device_id_type=MESH
        )
        copy.start()
        return copy

    first = iota((1, TILE), 1) < WIDTH
    smalls[0].wait()
    ld32[...] = jnp.zeros_like(ld32)
    ld32[0:HEADS, :] = ld_ref[...] * LOG2E
    cum = prefix_sums(ld32[...], False)
    for h in range(HEADS):
        lrow[h] = cum[h : h + 1, :]
    hi, mid, lo = split3(cum)
    stack = jnp.concatenate(
        [hi.astype(F32), mid.astype(F32), lo.astype(F32), jnp.zeros_like(cum)], axis=0
    )
    columns = stack.T
    zl3[spot] = columns[TOK - 1 : TOK, :]
    columns = columns.astype(BF16)
    narrow = (TILE, ROWS)
    spread = jnp.where((iota(narrow, 0) & 31) == (iota(narrow, 1) >> 6), 1.0, 0.0).astype(BF16)
    lanes[...] = spread
    smalls[1].wait()
    ct_pair = split(c_ref[...].T)

    def tile_of(p):
        return pl.ds(pl.multiple_of(p * TILE, TILE), TILE)

    def logs_of(p):
        return nn(columns, lanes[:, tile_of(p)])

    def starter(k):
        def start(p, carry):
            tile = tile_of(p + k * PART_PAIRS)
            e_pair = split(jnp.exp2(logs_of(p + k * PART_PAIRS)) * dy_ref[:, tile])
            eh[:, tile] = e_pair[0]
            el[:, tile] = e_pair[1]
            gt_ref[k, :, tile_of(p)] = nn3(ct_pair, e_pair)
            return carry

        return start

    away = pl.ds(pl.multiple_of((1 - core) * HALF, HALF), HALF)
    mine = pl.ds(pl.multiple_of(core * HALF, HALF), HALF)
    m_copies = []
    for k in range(PARTS):
        loads[k].wait()
        lax.fori_loop(0, PART_PAIRS, starter(k), 0)
        if k == 0:
            pl.semaphore_wait(barrier, len(everyone))
            l_copies = [
                send(zl3.at[spot], zl3.at[spot], l_s.at[d], l_r.at[d], peer(x, q // 2, lax.rem(q, 2)))
                for q, d in zip(line, range(LINE - 1))
            ]
        m_copies.append(send(gt_ref.at[k, away], pg.at[k], pair_s.at[0, k], pair_r.at[0, k], mate))
    rest = [
        pltpu.make_async_copy(x_hbm, x_ref, in_s.at[PARTS]),
        pltpu.make_async_copy(s0_hbm, s0_ref, in_s.at[PARTS + 1]),
    ]
    for load in rest:
        load.start()

    for copy in l_copies:
        copy.wait()
    line_logs = nn(jnp.concatenate([zl3[i] for i in range(LINE)], axis=0).astype(BF16), spread)
    log = jnp.zeros((1, ROWS), F32)
    for j in reversed(range(ZN)):
        one, two = line_logs[2 * j : 2 * j + 1], line_logs[2 * j + 1 : 2 * j + 2]
        zrow[2 * j] = one
        zrow[2 * j + 1] = two
        fac[j] = jnp.exp2(log)
        step[j] = jnp.exp2(one + two)
        log = log + (one + two)
    xl[x] = jnp.exp2(log)
    r_copies = [
        send(xl.at[x], xl.at[x], x_s.at[PARTS, d], x_r.at[PARTS, d], peer(q, z, core))
        for q, d in zip(x_peers, range(XN - 1))
    ]
    a0, a1 = jnp.exp2(zrow[2 * z]), jnp.exp2(zrow[2 * z + 1])
    a_ref[...] = jnp.where(even, a0, a1)

    z_copies = []
    for k in range(PARTS):
        m_copies[k].wait()
        for j in range(ZN):
            rows = pl.ds(pl.multiple_of(core * HALF + j * SLICE, SLICE), SLICE)
            part, mate_part = gt_ref[k, rows, :], pg[k, j * SLICE : (j + 1) * SLICE, :]
            later = jnp.where(even, mate_part, part)
            g1[k, j] = later
            chip[k, j] = jnp.where(even, part, mate_part) + a0[:, lanes_of(k)] * later
        z_copies.append(
            [
                send(chip.at[k, q], zbuf.at[k, z], z_s.at[k, d], z_r.at[k, d], peer(x, q, core))
                for q, d in zip(z_peers, range(ZN - 1))
            ]
        )
        zbuf[k, z] = chip[k, z]

    wide = (TILE, HEADS * TILE)
    spread = jnp.where((iota(wide, 0) & 31) == (iota(wide, 1) >> 7), 1.0, 0.0).astype(BF16)
    for k in range(HEADS // 4):
        part = slice(k * 4 * TILE, (k + 1) * 4 * TILE)
        lx[:, part] = nn(columns, spread[:, part])
    c_pair = split(c_ref[...])
    smalls[2].wait()
    b_pair = split(b_ref[...])
    causal = iota((TOK, TOK), 0) <= iota((TOK, TOK), 1)
    cbt[...] = jnp.where(causal, nt3(b_pair, c_pair), 0.0)
    et[...] = jnp.zeros_like(et)

    picker = jnp.concatenate([pair_picker()] * 2, axis=1)
    c_both = jnp.concatenate(c_pair, axis=1)
    b_both = jnp.concatenate(b_pair, axis=1)
    sub = iota((8, TOK), 0)

    def inner(p, carry):
        tile = tile_of(p)
        xv, dy = x_ref[:, tile], dy_ref[:, tile]
        both = logs_of(p)
        tail = jnp.exp2(both[TOK - 1 : TOK, :] - both)
        tail_ref[:, tile] = tail
        tx = split(tail * xv)
        txh[:, tile] = tx[0]
        txl[:, tile] = tx[1]
        xh, xlo = split(xv)
        dyh, dyl = split(dy)
        xh_f, dyh_f = xh.astype(F32), dyh.astype(F32)
        x_turn = pltpu.roll(xlo.astype(F32), WIDTH, 1)
        dy_turn = pltpu.roll(dyh_f, WIDTH, 1)
        dyl_f = dyl.astype(F32)
        zero = jnp.zeros_like(xv)
        dycat = jnp.concatenate([dyh, dyl], axis=1)
        left, right = [], []
        for k in range(2):
            here = first if k == 0 else jnp.logical_not(first)
            left.append(
                jnp.concatenate(
                    [jnp.where(here, xh_f, x_turn), jnp.where(here, xh_f, zero)], axis=1
                ).astype(BF16)
            )
            right.append(
                jnp.concatenate(
                    [jnp.where(here, dyh_f, dy_turn), jnp.where(here, dyl_f, zero)], axis=1
                ).astype(BF16)
            )
        zs = [[jnp.zeros((1, TILE), F32) for j in range(4)] for k in range(2)]
        blank = jnp.zeros((TILE, TILE), BF16)
        for i in range(2):
            r = i * 2 * TILE
            outs = []
            gained = [et[r + m * TILE : r + (m + 1) * TILE, r + m * TILE :] for m in range(2)]
            for k in range(2):
                grads = nt(left[k][r : r + 2 * TILE], right[k][r:])
                highs, lows = [], []
                for m in range(2):
                    q = r + m * TILE
                    grad = grads[m * TILE : (m + 1) * TILE, m * TILE :]
                    column = lx[q : q + TILE, tile_of(2 * p + k)]
                    row = lrow[2 * p + k][:, q:]
                    decay = []
                    for j in range((TOK - q) // TILE):
                        gap = row[:, j * TILE : (j + 1) * TILE] - column
                        decay.append(jnp.exp2(jnp.minimum(gap, 0.0) if j == 0 else gap))
                    decay = jnp.concatenate(decay, axis=1)
                    weight = decay * cbt[q : q + TILE, q:]
                    gained[m] = gained[m] + decay * grad
                    sums = jnp.sum(weight * grad, axis=0, keepdims=True)
                    for j in range((TOK - q) // TILE):
                        at = q // TILE + j
                        zs[k][at] = zs[k][at] + sums[:, j * TILE : (j + 1) * TILE]
                    wh, wl = split(weight)
                    highs.append(jnp.concatenate([blank, wh], axis=1) if m else wh)
                    lows.append(jnp.concatenate([blank, wl], axis=1) if m else wl)
                out = nn(jnp.concatenate(highs, axis=0), dycat[r:])
                low = nn(jnp.concatenate(lows, axis=0), dyh[r:])
                outs.append(out[:, :TILE] + out[:, TILE:] + low)
            for m in range(2):
                q = r + m * TILE
                et[q : q + TILE, q:] = gained[m]
            dx_ref[r : r + 2 * TILE, tile] = jnp.where(first, outs[0], outs[1])
        sh, sl = split(s0_ref[tile, :])
        both = nt(
            c_both,
            jnp.concatenate(
                [jnp.concatenate([sh, sh], axis=1), jnp.concatenate([sl, sl], axis=1)], axis=0
            ),
        )
        entering = both[:, :TILE] + both[:, TILE:]
        e = eh[:, tile].astype(F32) + el[:, tile].astype(F32)
        vh, vl = split(xv * dx_ref[:, tile] - e * entering)
        za, zb = jnp.concatenate(zs[0], axis=1), jnp.concatenate(zs[1], axis=1)
        v_ref[p] = (
            nt(picker, jnp.concatenate([vh, vl], axis=1))
            - jnp.where(sub == 0, za, jnp.where(sub == 1, zb, 0.0))
        )
        return carry

    for load in rest:
        load.wait()

    def line_scan(k):
        for copy in z_copies[k]:
            copy.wait()
        state = jnp.zeros((SLICE, PART), F32)
        for j in reversed(range(ZN)):
            inside[k, j] = state
            state = zbuf[k, j] + step[j][:, lanes_of(k)] * state
        xg[k, x] = state
        return [
            send(xg.at[k, x], xg.at[k, x], x_s.at[k, d], x_r.at[k, d], peer(q, z, core))
            for q, d in zip(x_peers, range(XN - 1))
        ]

    def line_back(k, copies):
        for copy in copies:
            copy.wait()
        entering = jnp.zeros((SLICE, PART), F32)
        for q in reversed(range(1, XN)):
            entering = jnp.where(q > x, xg[k, q] + xl[q][:, lanes_of(k)] * entering, entering)
        for j in range(ZN):
            lbuf[k, j] = inside[k, j] + fac[j][:, lanes_of(k)] * entering
        copies = [
            send(lbuf.at[k, q], back.at[k, z], b_s.at[k, d], b_r.at[k, d], peer(x, q, core))
            for q, d in zip(z_peers, range(ZN - 1))
        ]
        back[k, z] = lbuf[k, z]
        return copies

    lax.fori_loop(0, CUTS[0], inner, 0)
    x_copies = [line_scan(0)]
    lax.fori_loop(CUTS[0], CUTS[1], inner, 0)
    for copy in r_copies:
        copy.wait()
    b_copies = [line_back(0, x_copies[0])]
    lax.fori_loop(CUTS[1], CUTS[2], inner, 0)
    x_copies.append(line_scan(1))
    lax.fori_loop(CUTS[2], CUTS[3], inner, 0)
    b_copies.append(line_back(1, x_copies[1]))
    lax.fori_loop(CUTS[3], PAIRS, inner, 0)

    part = TOK // HN
    here = pl.ds(pl.multiple_of(hd * part, part), part)

    def scatter(own, got, k):
        return [
            send(own.at[q], got.at[d], y_s.at[k, d], y_r.at[k, d], (me, q))
            for q, d in zip(y_peers, range(HN - 1))
        ]

    def gather(own, got, out, k):
        out[here, :] = own[hd] + got[0] + got[1] + got[2]
        return [
            send(out.at[here], out.at[here], y_s.at[k, d], y_r.at[k, d], (me, q))
            for q, d in zip(y_peers, range(HN - 1))
        ]

    table = jnp.where(causal, et[...], 0.0)
    s_pair = split(s0_ref[...])
    dc = nn3(split(table.T), b_pair) + nn3((eh[...], el[...]), s_pair)
    for q in range(HN):
        own_c[q] = dc[q * part : (q + 1) * part]
    c_copies = scatter(own_c, got_c, 0)
    dbl[...] = nn3(split(table), c_pair)

    f_copies = []
    for k in range(PARTS):
        for copy in b_copies[k]:
            copy.wait()
        for j in range(ZN):
            late = back[k, j]
            early = g1[k, j] + a1[:, lanes_of(k)] * late
            rows = pl.ds(pl.multiple_of(core * HALF + j * SLICE, SLICE), SLICE)
            lat[k, rows, :] = jnp.where(even, early, late)
            other[k, j * SLICE : (j + 1) * SLICE, :] = jnp.where(even, late, early)
        f_copies.append(
            send(other.at[k], lat.at[k, mine], pair_s.at[1, k], pair_r.at[1, k], mate)
        )
    for copy in c_copies:
        copy.wait()
    c_copies = gather(own_c, got_c, dc_ref, 1)
    db = dbl[...]
    for k in range(PARTS):
        f_copies[k].wait()
        hi, lo = split(lat[k])
        lh[k] = hi
        ll[k] = lo
        both = nt(txh[:, lanes_of(k)], jnp.concatenate([hi, lo], axis=0))
        db = db + both[:, :STATE] + both[:, STATE:] + nt(txl[:, lanes_of(k)], hi)
    for q in range(HN):
        own_b[q] = db[q * part : (q + 1) * part]
    d_copies = scatter(own_b, got_b, 2)

    top = iota((8, TILE), 0)

    def corrector(k):
        def correct(p, carry):
            tile = tile_of(p + k * PART_PAIRS)
            spot = tile_of(p)
            late = jnp.concatenate([lh[k, :, spot], ll[k, :, spot]], axis=1)
            raw = nn(b_both, jnp.concatenate([late, late], axis=0))
            raw = raw[:, :TILE] + raw[:, TILE:]
            dx_ref[:, tile] = dx_ref[:, tile] + tail_ref[:, tile] * raw
            tx = txh[:, tile].astype(F32) + txl[:, tile].astype(F32)
            vh, vl = split(tx * raw)
            slot = pl.ds(pl.multiple_of((p + k * PART_PAIRS) * 8, 8), 8)
            w[slot, :] = v_ref[p + k * PART_PAIRS] + nt(
                picker, jnp.concatenate([vh, vl], axis=1)
            )
            eg = (a_ref[:, tile] * lat[k, :, spot] + gt_ref[k, :, spot]).T
            eg_ref[tile, :] = eg
            product = eg * s0_ref[tile, :]
            one = jnp.sum(jnp.sum(product[:WIDTH], axis=0, keepdims=True), axis=1, keepdims=True)
            two = jnp.sum(jnp.sum(product[WIDTH:], axis=0, keepdims=True), axis=1, keepdims=True)
            first_g[slot, :] = jnp.where(top == 0, one, jnp.where(top == 1, two, 0.0))
            return carry

        return correct

    lax.fori_loop(0, PART_PAIRS, corrector(0), 0)
    for copy in d_copies:
        copy.wait()
    d_copies = gather(own_b, got_b, db_ref, 3)
    lax.fori_loop(0, PART_PAIRS, corrector(1), 0)
    rates = prefix_sums(w[...], True) + first_g[:, 0:1]
    for h in range(HEADS):
        k = (h // 2) * 8 + h % 2
        dld_ref[h : h + 1, :] = rates[k : k + 1, :]
    for copy in c_copies:
        copy.wait()
    for copy in d_copies:
        copy.wait()


def run(x, ld, b, c, s0, dy):
    vm = pl.BlockSpec(memory_space=pltpu.VMEM)
    hbm = pl.BlockSpec(memory_space=pltpu.HBM)
    dma = pltpu.SemaphoreType.DMA
    shape = jax.ShapeDtypeStruct
    slab = pltpu.VMEM((PARTS, ZN, SLICE, PART), F32)
    half = pltpu.VMEM((PARTS, HALF, PART), F32)
    rows8 = pltpu.VMEM((ZN, 1, ROWS), F32)
    tall = pltpu.VMEM((TOK, ROWS), F32)
    tall16 = pltpu.VMEM((TOK, ROWS), BF16)
    state = pltpu.VMEM((PARTS, STATE, PART), F32)
    state16 = pltpu.VMEM((PARTS, STATE, PART), BF16)
    quarter = TOK // HN
    return pl.pallas_call(
        main_kernel,
        out_shape=(
            pltpu.VMEM((TOK, ROWS), F32),
            pltpu.VMEM((HEADS, TOK), F32),
            pltpu.VMEM((TOK, STATE), F32),
            pltpu.VMEM((TOK, STATE), F32),
            pltpu.VMEM((ROWS, STATE), F32),
        ),
        in_specs=[hbm] * 6,
        out_specs=(vm,) * 5,
        scratch_shapes=[
            tall,
            pltpu.VMEM((ROWS, STATE), F32),
            tall,
            state,
            pltpu.VMEM((1, ROWS), F32),
            tall16,
            tall16,
            tall,
            pltpu.VMEM((PAIRS, 8, TOK), F32),
            pltpu.VMEM((TOK, STATE), F32),
            pltpu.VMEM((HEADS, TOK), F32),
            pltpu.VMEM((TOK, STATE), F32),
            pltpu.VMEM((TOK, STATE), F32),
            pltpu.VMEM((32, TOK), F32),
            pltpu.VMEM((TILE, ROWS), BF16),
            pltpu.VMEM((TOK, HEADS * TILE), F32),
            pltpu.VMEM((HEADS, 1, TOK), F32),
            pltpu.VMEM((TOK, TOK), F32),
            pltpu.VMEM((TOK, TOK), F32),
            tall16,
            tall16,
            half,
            slab,
            slab,
            slab,
            pltpu.VMEM((LINE, 1, TILE), F32),
            pltpu.VMEM((LINE, 1, ROWS), F32),
            slab,
            rows8,
            rows8,
            pltpu.VMEM((PARTS, XN, SLICE, PART), F32),
            pltpu.VMEM((XN, 1, ROWS), F32),
            slab,
            slab,
            half,
            state,
            state16,
            state16,
            pltpu.VMEM((PAIRS * 8, TOK), F32),
            pltpu.VMEM((PAIRS * 8, TILE), F32),
            pltpu.VMEM((HN, quarter, STATE), F32),
            pltpu.VMEM((HN - 1, quarter, STATE), F32),
            pltpu.VMEM((HN, quarter, STATE), F32),
            pltpu.VMEM((HN - 1, quarter, STATE), F32),
            dma((PARTS + 5,)),
            dma((2, PARTS)), dma((2, PARTS)),
            dma((LINE - 1,)), dma((LINE - 1,)),
            dma((PARTS, ZN - 1)), dma((PARTS, ZN - 1)),
            dma((PARTS + 1, XN - 1)), dma((PARTS + 1, XN - 1)),
            dma((PARTS, ZN - 1)), dma((PARTS, ZN - 1)),
            dma((4, HN - 1)), dma((4, HN - 1)),
        ],
        compiler_params=pltpu.CompilerParams(
            collective_id=0, has_side_effects=True, vmem_limit_bytes=VMEM_LIMIT
        ),
        name="main",
    )(x, ld, b, c, s0, dy)


def out_kernel(*refs):
    sem = refs[-1]
    half = (len(refs) - 1) // 2
    copies = [
        pltpu.make_async_copy(refs[k], refs[half + k], sem.at[k]) for k in range(half)
    ]
    for copy in copies:
        copy.start()
    for copy in copies:
        copy.wait()


def store(*values):
    return pl.pallas_call(
        out_kernel,
        out_shape=tuple(jax.ShapeDtypeStruct(v.shape, v.dtype) for v in values),
        in_specs=[pl.BlockSpec(memory_space=pltpu.VMEM)] * len(values),
        out_specs=(pl.BlockSpec(memory_space=pltpu.HBM),) * len(values),
        scratch_shapes=[pltpu.SemaphoreType.DMA((len(values),))],
        compiler_params=pltpu.CompilerParams(vmem_limit_bytes=1024 * 1024),
        name="store",
    )(*values)


def per_device(inputs, log_decay, b_proj, c_proj, entry_states, out_grad):
    s0 = entry_states.reshape(ROWS, STATE)
    dx, dld, db, dc, eg = store(*run(inputs, log_decay, b_proj, c_proj, s0, out_grad))
    return (dx, dld, db, dc, eg.reshape(1, HEADS, WIDTH, STATE))


def solution(mesh):
    return jax.shard_map(
        per_device,
        mesh=mesh,
        in_specs=(
            P("seq", "head"),
            P("head", "seq"),
            P("seq", None),
            P("seq", None),
            P("seq", "head", None, None),
            P("seq", "head"),
        ),
        out_specs=(
            P("seq", "head"),
            P("head", "seq"),
            P("seq", None),
            P("seq", None),
            P("seq", "head", None, None),
        ),
        check_vma=False,
    )
```
